128 devices in a mesh: chan: 4 (over y), tm: 32 (over z, x, core).
Axes of the slice: x: 4, y: 4, z: 4, core: 2. Of those that a mesh axis runs over, the one named last changes fastest.
Arguments:
- strain: float32 [768, 524288], P('chan', 'tm'), may hold values from -6 to 6
Outputs:
- power: float32 [768, 8192], P('chan', 'tm')
- nyquist: float32 [768], P('chan')
- mean_power: float32 [8192], P('tm')
The draws below stay inside these ranges and needn't reach their ends.
All inputs are finite; a program needn't handle non-finite values.
Results may differ from the reference program's by a relative error of at most 0.00007.
Values sent between devices are 32-bit elements; how exact they have to be, the bound alone decides.
A program may use at most 192 MiB of HBM per device.

```python
import jax
import jax.numpy as jnp
from jax import lax

SEG = 16384
HOP = 8192
BINS = 8192
CHANNELS = 768
SAMPLES = 524288
SEGMENTS = 63


def level_of(stream_key, extent, split, low, top_value):
    loudness = 1.0
    for dim, shards_of in split:
        draws = jax.random.uniform(jax.random.fold_in(jax.random.fold_in(stream_key, 6), dim), (shards_of,), jnp.float32, low / len(split), top_value / len(split))
        loudness = loudness * jnp.repeat(jnp.exp(draws), extent[dim] // shards_of).reshape((-1,) + (1,) * (len(extent) - 1 - dim))
    return loudness


def bell_draw(key, dims, spread, most, cuts=(), kind=jnp.bfloat16):
    drawn = jax.random.normal(key, dims, jnp.float32) * spread
    if len(cuts) > 0:
        drawn = level_of(key, dims, cuts, -0.22, 0.18) * drawn
    return jnp.clip(drawn, min=-most, max=most).astype(kind)


def setup_inputs(seed: int = 0) -> dict:
    keys = jax.random.split(jax.random.key(seed), 2)
    strain = bell_draw(keys[0], (CHANNELS, SAMPLES), 1.0, 6.0, ((0, 4), (1, 32)), jnp.float32)
    return dict(strain=strain)


def hann_window():
    sample_pos = jnp.arange(SEG, dtype=jnp.float32)
    return 0.5 - 0.5 * jnp.cos(2.0 * jnp.pi * sample_pos / SEG)


def reference(strain):
    window = hann_window()
    energy = jnp.sum(window * window)

    def one_channel(signal):
        blocks = signal.reshape(SEGMENTS + 1, HOP)
        pieces = jnp.concatenate([blocks[:-1], blocks[1:]], axis=1)
        centred = (pieces - jnp.mean(pieces, axis=1, keepdims=True)) * window
        spectrum = jnp.fft.rfft(centred, axis=1)
        return jnp.sum(jnp.real(spectrum) ** 2 + jnp.imag(spectrum) ** 2, axis=0)

    totals = lax.map(one_channel, strain)
    doubling = jnp.where(jnp.arange(BINS) == 0, 1.0, 2.0).astype(totals.dtype)
    power = totals[:, :BINS] * doubling / (SEGMENTS * energy)
    nyquist = totals[:, BINS] / (SEGMENTS * energy)
    mean_power = jnp.mean(power, axis=0)
    return power, nyquist, mean_power
```

```python
import functools

import jax
import jax.numpy as jnp
import numpy as np
from jax import lax
from jax.experimental import pallas as pl
from jax.experimental.pallas import tpu as pltpu
from jax.sharding import PartitionSpec as P

ROOT = 128
HALF = ROOT // 2
ROWS = 8


def split_np(table):
    table = table.astype(np.float32)
    high = table.astype(jnp.bfloat16)
    low = (table - high.astype(np.float32)).astype(jnp.bfloat16)
    return high, low


@functools.cache
def tables(tm_count):
    pos = np.arange(ROOT)
    short = 2.0 * np.pi * (np.outer(pos, pos) % ROOT) / ROOT
    cos_s, sin_s = np.cos(short), np.sin(short)
    first = np.concatenate([cos_s[:HALF], -sin_s[:HALF]], axis=0)
    first_hi, first_lo = split_np(first)
    first_all = np.concatenate(
        [
            np.concatenate([first_hi, first_hi], axis=1),
            np.concatenate([first_lo, first_lo], axis=1),
        ],
        axis=0,
    )
    bands = np.arange(HALF).reshape(tm_count, HALF // tm_count)
    order = np.concatenate([bands, ROOT - 1 - bands], axis=1).reshape(-1)
    cos_o, sin_o = cos_s[:, order], sin_s[:, order]
    second = np.concatenate(
        [np.concatenate([cos_o, -sin_o], axis=1), np.concatenate([sin_o, cos_o], axis=1)], axis=0
    )
    second_hi, second_lo = split_np(second)
    second_all = np.concatenate([second_hi, second_hi, second_lo], axis=0)
    long = 2.0 * np.pi * np.outer(np.arange(HALF + ROWS), pos) / (ROOT * ROOT)
    twist = np.concatenate([np.cos(long), np.sin(long)], axis=1).astype(np.float32)
    mirror = np.zeros((2 * ROOT, 2 * ROOT), np.float32)
    for side in range(2):
        for k in range(HALF):
            mirror[side * HALF + k, side * ROOT + k] = 1.0
            mirror[ROOT + side * HALF + k, side * ROOT + (ROOT - k if k else HALF)] = 1.0
    seg_len = ROOT * ROOT
    window = 0.5 - 0.5 * np.cos(2.0 * np.pi * np.arange(seg_len) / seg_len)
    energy = float(np.sum(window * window))
    return first_all, second_all, twist, window.reshape(ROOT, ROOT).astype(np.float32), mirror, energy


def split(value):
    high = value.astype(jnp.bfloat16)
    low = (value - high.astype(jnp.float32)).astype(jnp.bfloat16)
    return high, low


SPAN = 4
CORES = 2


def half_sum(ref, offset):
    parts = [ref[:, offset + ROOT * a : offset + ROOT * (a + 1)] for a in range(HALF)]
    while len(parts) > 1:
        parts = [parts[n] + parts[n + 1] for n in range(0, len(parts), 2)]
    return jnp.sum(parts[0], axis=1, keepdims=True)


def stage_one(parts, mean, consts, buf, zbuf, ebuf, seg, segs, erow):
    window_ref, first_ref, _, twist_ref = consts
    mean = jnp.broadcast_to(mean, (ROWS, ROOT))
    even = jnp.zeros((ROWS, ROOT), jnp.float32)
    odd = jnp.zeros((ROWS, ROOT), jnp.float32)
    for a in range(ROOT):
        ref, offset = parts[a // HALF]
        start = offset + ROOT * (a % HALF)
        tile = (ref[:, start : start + ROOT] - mean) * window_ref[a : a + 1, :]
        buf[ROWS * a : ROWS * (a + 1), :] = tile
        if a % 2 == 0:
            even = even + tile
        else:
            odd = odd + tile
    alt = even - odd
    sign = (1 - 2 * (lax.broadcasted_iota(jnp.int32, (ROWS, ROOT), 1) % 2)).astype(jnp.float32)
    edge = jnp.sum((even + odd) * sign, axis=1, keepdims=True)
    turn = twist_ref[HALF : HALF + 1, :]
    high, low = split(jnp.concatenate([alt * turn[:, :ROOT], -alt * turn[:, ROOT:]], axis=1))
    ebuf[erow : erow + ROWS, :] = jnp.concatenate([high, low, high], axis=1)
    cos_t, sin_t = twist_ref[:HALF, :ROOT], twist_ref[:HALF, ROOT:]
    for r in range(0, ROWS, 2):
        pair = jnp.concatenate(
            [buf[pl.ds(r, ROOT, stride=ROWS), :], buf[pl.ds(r + 1, ROOT, stride=ROWS), :]], axis=1
        )
        high, low = split(pair)
        out = jnp.dot(
            first_ref[...], jnp.concatenate([high, low], axis=0), preferred_element_type=jnp.float32
        )
        out = out[:ROOT] + out[ROOT:]
        for s in range(2):
            re = out[:HALF, s * ROOT : (s + 1) * ROOT]
            im = out[HALF:, s * ROOT : (s + 1) * ROOT]
            z_hi, z_lo = split(
                jnp.concatenate([re * cos_t + im * sin_t, im * cos_t - re * sin_t], axis=1)
            )
            at = ((r + s) * segs + seg) * HALF
            zbuf[at : at + HALF, 0 : 2 * ROOT] = z_hi
            zbuf[at : at + HALF, 2 * ROOT :] = z_lo
    return edge * edge


def squares(left, right):
    out = jnp.dot(left, right, preferred_element_type=jnp.float32)
    return out[:, :ROOT] * out[:, :ROOT] + out[:, ROOT:] * out[:, ROOT:]


def side_sums(side, own, halo, on, wait_halo, consts, scratch):
    second_ref = consts[2]
    buf, zbuf, ebuf, psum = scratch
    half_len = ROOT * HALF
    segs = 2 * CORES
    lane = lax.broadcasted_iota(jnp.int32, (ROWS, ROOT), 1)
    pieces = [(own, half_len * h) for h in range(segs)]
    totals = [half_sum(*piece) for piece in pieces]
    inverse = 1.0 / (2 * half_len)
    nyq = jnp.zeros((ROWS, 1), jnp.float32)
    for seg in range(segs - 1):
        nyq = nyq + stage_one(
            (pieces[seg], pieces[seg + 1]), (totals[seg] + totals[seg + 1]) * inverse,
            consts, buf, zbuf, ebuf, seg, segs, seg * ROWS,
        )
    wait_halo()
    far = (halo, 0)
    straddle = (pieces[-1], far) if side == 0 else (far, pieces[0])
    near = totals[-1] if side == 0 else totals[0]
    nyq = nyq + on * stage_one(
        straddle, (near + half_sum(*far)) * inverse, consts, buf, zbuf, ebuf, segs - 1, segs, (segs - 1) * ROWS
    )

    def fold(power, rows):
        total = power[:rows]
        for seg in range(1, segs - 1):
            total = total + power[seg * rows : (seg + 1) * rows]
        return total + on * power[(segs - 1) * rows :]

    for r in range(ROWS):
        rows = slice(r * segs * HALF, (r + 1) * segs * HALF)
        left = jnp.concatenate([zbuf[rows, :], zbuf[rows, : 2 * ROOT]], axis=1)
        at = r * ROOT + side * HALF
        psum[at : at + HALF, :] = fold(squares(left, second_ref[...]), HALF)
    mixed = fold(squares(ebuf[...], second_ref[...]), ROWS)
    first_rows = pl.ds(side * HALF, ROWS, stride=ROOT)
    psum[first_rows, :] = jnp.where(lane % SPAN >= SPAN // 2, mixed, psum[first_rows, :])
    return nyq


def welch_kernel(
    scale, strain_ref, window_ref, first_ref, second_ref, twist_ref, mirror_ref,
    power_ref, nyquist_ref, mean_ref,
    data, halo, sums, fin, from_partner, z_in, x_in, nyq_rows, nyq_out, nyq_in, nyq_partner,
    buf, zbuf, ebuf, psum, channel_sums, channel_from,
    load_sem, swap_send, swap_recv, halo_send, halo_recv,
    z_send, z_recv, x_send, x_recv, core_send, core_recv,
    nyq_send, nyq_recv, nyq_core_send, nyq_core_recv, chan_send, chan_recv,
):
    chan, chan_count = lax.axis_index("chan"), lax.axis_size("chan")
    me = lax.axis_index("tm")
    core = lax.rem(me, CORES)
    chip = me // CORES
    chips = lax.axis_size("tm") // CORES
    z, x = chip // SPAN, lax.rem(chip, SPAN)
    half_len = ROOT * HALF
    block_len = 2 * half_len
    mine = data.shape[0]
    wide = 2 * ROWS
    steps = mine // wide
    has_left, has_right = chip > 0, chip < chips - 1
    exists = (has_right, has_left)
    on = [flag.astype(jnp.float32) for flag in exists]

    def device(chip_index, core_index):
        return {"tm": chip_index * CORES + core_index}

    def z_peer(step):
        return device(lax.rem(z + step + SPAN, SPAN) * SPAN + x, core)

    def x_peer(step):
        return device(z * SPAN + lax.rem(x + step + SPAN, SPAN), core)

    partner = device(chip, 1 - core)

    def remote(source, target, send, recv, where):
        return pltpu.make_async_remote_copy(
            src_ref=source, dst_ref=target, send_sem=send, recv_sem=recv,
            device_id=where, device_id_type=pl.DeviceIdType.MESH,
        )

    columns = pl.ds(pl.multiple_of(core * block_len, block_len), block_len)

    def strip(i):
        return pl.ds(pl.multiple_of(i * wide, wide), wide)

    def load(i):
        rows = pl.ds(pl.multiple_of(core * mine + i * wide, wide), wide)
        return pltpu.make_async_copy(strain_ref.at[rows], data.at[strip(i), columns], load_sem.at[i])

    def swap(i):
        rows = pl.ds(pl.multiple_of((1 - core) * mine + i * wide, wide), wide)
        return remote(
            strain_ref.at[rows], data.at[strip(i), columns], swap_send.at[i], swap_recv.at[i], partner
        )

    def halo_copy(i, to):
        at = pl.multiple_of(i * wide + core * ROWS, ROWS)
        source = strain_ref.at[
            pl.ds(pl.multiple_of(to * mine + at, ROWS), ROWS),
            pl.ds(pl.multiple_of(core * half_len, half_len), half_len),
        ]
        return remote(
            source, halo.at[pl.ds(at, ROWS)], halo_send.at[to, i], halo_recv.at[core, i],
            device(chip - 1 + 2 * core, to),
        )

    def halo_arrival(i, side):
        block = halo.at[pl.ds(pl.multiple_of(i * wide + side * ROWS, ROWS), ROWS)]
        return remote(block, block, halo_send.at[0, i], halo_recv.at[side, i], partner)

    sends_halo = jnp.where(core == 0, has_left.astype(jnp.int32), has_right.astype(jnp.int32)) == 1

    @pl.loop(0, steps)
    def _(i):
        load(i).start()

    barrier = pltpu.get_barrier_semaphore()

    def greet(where):
        pl.semaphore_signal(barrier, inc=1, device_id=where, device_id_type=pl.DeviceIdType.MESH)

    greet(partner)
    for k in range(1, SPAN):
        greet(z_peer(k))
        greet(x_peer(k))
    for k in range(1, chan_count):
        greet({"chan": lax.rem(chan + k, chan_count)})
    for flag, shift, both in ((has_left, -1, 0), (has_right, 1, 1)):
        @pl.when(flag)
        def _():
            greet(device(chip + shift, 1 - both))

            @pl.when(core == both)
            def _():
                greet(device(chip + shift, both))
    left_count = has_left.astype(jnp.int32) * (2 - core)
    right_count = has_right.astype(jnp.int32) * (1 + core)
    pl.semaphore_wait(barrier, left_count + right_count + 1 + 2 * (SPAN - 1) + chan_count - 1)

    @pl.loop(0, steps)
    def _(i):
        swap(i).start()

        @pl.when(sends_halo)
        def _():
            for to in range(CORES):
                halo_copy(i, to).start()

    nyq_rows[...] = jnp.zeros_like(nyq_rows)
    consts = (window_ref, first_ref, second_ref, twist_ref)
    scratch = (buf, zbuf, ebuf, psum)

    def slab(i):
        return pl.ds(pl.multiple_of(i * ROWS, ROWS), ROWS)

    def way(i):
        return 1 - 2 * lax.rem(i, 2)

    def z_block(i, step):
        return sums.at[slab(i), lax.rem(z + step + SPAN, SPAN)]

    def x_block(i, step):
        return sums.at[slab(i), z, lax.rem(x + step + SPAN, SPAN)]

    def z_copy(kind, i):
        d = way(i)
        block, hop = ((2, d), (-d, -d), (d, d))[kind]
        return remote(z_block(i, block), z_in.at[kind, i], z_send.at[kind, i], z_recv.at[kind, i], z_peer(hop))

    def x_copy(kind, i):
        d = way(i)
        block, hop = ((2, d), (-d, -d), (d, d))[kind]
        return remote(x_block(i, block), x_in.at[kind, i], x_send.at[kind, i], x_recv.at[kind, i], x_peer(hop))

    def core_copy(i):
        rows = pl.ds(pl.multiple_of(i * ROWS * ROWS, ROWS * ROWS), ROWS * ROWS)
        return remote(fin.at[rows], from_partner.at[rows], core_send.at[i], core_recv.at[i], partner)

    def advance(copy, block, inbox, i):
        copy(0, i).wait_recv()
        target = block(i, way(i))
        target[...] = target[...] + inbox[0, i]
        copy(2, i).start()

    def collect(copy, block, inbox, i):
        copy(1, i).wait_recv()
        copy(2, i).wait_recv()
        return block(i, 0)[...] + inbox[1, i] + inbox[2, i]

    def nyq_copy(level, k):
        where = (z_peer, x_peer)[level](k)
        return remote(nyq_out.at[level], nyq_in.at[level, k], nyq_send.at[level, k], nyq_recv.at[level, k], where)

    def nyq_final():
        return remote(nyq_out.at[2], nyq_partner, nyq_core_send, nyq_core_recv, partner)

    @pl.loop(0, steps + 4)
    def _(t):
        @pl.when(t < steps)
        def _():
            load(t).wait()
            swap(t).wait_recv()
            for side in range(2):
                part = pl.ds(pl.multiple_of(t * wide + side * ROWS, ROWS), ROWS)

                def wait_halo():
                    @pl.when(exists[side])
                    def _():
                        halo_arrival(t, side).wait_recv()

                    @pl.when(jnp.logical_not(exists[side]))
                    def _():
                        halo[part, :] = jnp.zeros((ROWS, half_len), jnp.float32)

                nyq = side_sums(side, data.at[part], halo.at[part], on[side], wait_halo, consts, scratch)
                nyq_rows[part, :] = jnp.broadcast_to(nyq, (ROWS, ROOT))
            for r in range(ROWS):
                turned = jnp.transpose(psum[r * ROOT : (r + 1) * ROOT, :])
                sums[t * ROWS + r] = turned.reshape(sums.shape[1:])
            z_copy(0, t).start()
            z_copy(1, t).start()

        @pl.when(t == steps - 1)
        def _():
            turned = jnp.transpose(nyq_rows[...])
            nyq_out[0] = turned[:ROWS]
            for k in range(1, SPAN):
                nyq_copy(0, k).start()

        @pl.when(t >= 4)
        def _():
            i = t - 4
            fin[pl.ds(pl.multiple_of(i * ROWS * ROWS, ROWS * ROWS), ROWS * ROWS), :] = collect(
                x_copy, x_block, x_in, i
            ).reshape(ROWS * ROWS, ROOT)
            core_copy(i).start()

        @pl.when(jnp.logical_and(t >= 3, t < steps + 3))
        def _():
            advance(x_copy, x_block, x_in, t - 3)

        @pl.when(jnp.logical_and(t >= 2, t < steps + 2))
        def _():
            i = t - 2
            z_block(i, 0)[...] = collect(z_copy, z_block, z_in, i)
            x_copy(0, i).start()
            x_copy(1, i).start()

        @pl.when(jnp.logical_and(t >= 1, t < steps + 1))
        def _():
            advance(z_copy, z_block, z_in, t - 1)

        for level in range(2):
            @pl.when(t == steps + level)
            def _():
                total = nyq_out[level]
                for k in range(1, SPAN):
                    nyq_copy(level, k).wait_recv()
                    total = total + nyq_in[level, k]
                nyq_out[level + 1] = total
                if level == 0:
                    for k in range(1, SPAN):
                        nyq_copy(1, k).start()
                else:
                    nyq_final().start()

    nyq_final().wait_recv()
    for source in range(CORES):
        row = jnp.where(core == source, nyq_out[2], nyq_partner[...])
        nyquist_ref[source : source + 1, :] = row[:1] * scale

    lanes = lax.broadcasted_iota(jnp.int32, (1, ROOT), 1)
    column = [jnp.zeros((1, ROOT), jnp.float32) for _ in range(2)]
    for which, block in enumerate((fin, from_partner)):
        if which == 1:
            @pl.loop(0, steps)
            def _(i):
                core_copy(i).wait_recv()
        base = (core if which == 0 else 1 - core) * mine
        count = block.shape[0] // ROWS
        for j in range(2):
            both = jnp.concatenate(
                [
                    block[pl.ds(SPAN * core + j, count, stride=ROWS), :],
                    block[pl.ds(SPAN * core + 2 + j, count, stride=ROWS), :],
                ],
                axis=1,
            )
            placed = jnp.dot(
                both, mirror_ref[...], precision=lax.Precision.HIGHEST, preferred_element_type=jnp.float32
            )
            factor = jnp.where(jnp.logical_and(lanes == 0, me + j == 0), scale, 2.0 * scale)
            for side in range(2):
                value = placed[:, side * ROOT : (side + 1) * ROOT] * factor
                column[j] = column[j] + jnp.sum(value, axis=0, keepdims=True)
                for i in range(count // ROWS):
                    rows = pl.ds(pl.multiple_of(base + i * wide + side * ROWS, ROWS), ROWS)
                    power_ref[rows, j * ROOT : (j + 1) * ROOT] = value[i * ROWS : (i + 1) * ROWS]
    for j in range(2):
        channel_sums[j : j + 1, :] = column[j]

    def chan_copy(k):
        return remote(
            channel_sums, channel_from.at[k], chan_send.at[k], chan_recv.at[k],
            {"chan": lax.rem(chan + k, chan_count)},
        )

    for k in range(1, chan_count):
        chan_copy(k).start()

    @pl.loop(0, steps)
    def _(i):
        swap(i).wait_send()
        core_copy(i).wait_send()

        @pl.when(sends_halo)
        def _():
            for to in range(CORES):
                halo_copy(i, to).wait_send()

        for kind in range(3):
            z_copy(kind, i).wait_send()
            x_copy(kind, i).wait_send()

    for level in range(2):
        for k in range(1, SPAN):
            nyq_copy(level, k).wait_send()
    nyq_final().wait_send()

    channel_from[0] = channel_sums[...]
    for k in range(1, chan_count):
        chan_copy(k).wait()
    total = jnp.zeros_like(channel_sums)
    for source in range(chan_count):
        total = total + channel_from[lax.rem(chan - source + chan_count, chan_count)]
    mean_ref[...] = total * (1.0 / (CORES * mine * chan_count))


def per_device(strain):
    chan_rows, time_width = strain.shape
    seg_len = ROOT * ROOT
    half_len = seg_len // 2
    tm_count = lax.axis_size("tm")
    wide = 2 * ROWS
    mine = chan_rows // CORES
    assert time_width == seg_len and tm_count == SPAN * SPAN * CORES and mine % wide == 0 and mine <= ROOT
    segments = 2 * tm_count - 1
    band = half_len // tm_count
    first_all, second_all, twist, window, mirror, energy = tables(tm_count)
    pairs = mine // 2
    steps = mine // wide
    chan_count = lax.axis_size("chan")
    vmem = pl.BlockSpec(memory_space=pltpu.VMEM)
    f32 = jnp.float32
    dma = pltpu.SemaphoreType.DMA
    power, nyquist, mean_power = pl.pallas_call(
        functools.partial(welch_kernel, 1.0 / (segments * energy)),
        in_specs=[pl.BlockSpec(memory_space=pl.ANY)] + [vmem] * 5,
        out_specs=[vmem] * 3,
        out_shape=[
            jax.ShapeDtypeStruct((chan_rows, band), f32),
            jax.ShapeDtypeStruct((CORES, ROOT), f32),
            jax.ShapeDtypeStruct((2, ROOT), f32),
        ],
        scratch_shapes=[
            pltpu.VMEM((mine, CORES * seg_len), f32),
            pltpu.VMEM((mine, half_len), f32),
            pltpu.VMEM((pairs, SPAN, SPAN, ROWS, ROOT), f32),
            pltpu.VMEM((pairs * ROWS, ROOT), f32),
            pltpu.VMEM((pairs * ROWS, ROOT), f32),
            pltpu.VMEM((3, steps, ROWS, SPAN, ROWS, ROOT), f32),
            pltpu.VMEM((3, steps, ROWS, ROWS, ROOT), f32),
            pltpu.VMEM((ROOT, ROOT), f32),
            pltpu.VMEM((3, ROWS, ROOT), f32),
            pltpu.VMEM((2, SPAN, ROWS, ROOT), f32),
            pltpu.VMEM((ROWS, ROOT), f32),
            pltpu.VMEM((ROWS * ROOT, ROOT), f32),
            pltpu.VMEM((ROWS * 2 * CORES * HALF, 4 * ROOT), jnp.bfloat16),
            pltpu.VMEM((2 * CORES * ROWS, 6 * ROOT), jnp.bfloat16),
            pltpu.VMEM((ROWS * ROOT, ROOT), f32),
            pltpu.VMEM((2, ROOT), f32),
            pltpu.VMEM((chan_count, 2, ROOT), f32),
            dma((steps,)),
            dma((steps,)),
            dma((steps,)),
            dma((CORES, steps)),
            dma((2, steps)),
            dma((3, steps)),
            dma((3, steps)),
            dma((3, steps)),
            dma((3, steps)),
            dma((steps,)),
            dma((steps,)),
            dma((2, SPAN)),
            dma((2, SPAN)),
            dma(()),
            dma(()),
            dma((chan_count,)),
            dma((chan_count,)),
        ],
        compiler_params=pltpu.CompilerParams(
            collective_id=0, has_side_effects=True, vmem_limit_bytes=60 * 2**20
        ),
        name="welch",
    )(strain, window, first_all, second_all, twist, mirror)
    return (power, nyquist[:, :mine].reshape(-1), mean_power.reshape(-1))


def solution(mesh):
    in_specs = (P("chan", "tm"),)
    out_specs = (P("chan", "tm"), P("chan"), P("tm"))
    return jax.shard_map(
        per_device, mesh=mesh, in_specs=in_specs, out_specs=out_specs, check_vma=False
    )
```

```python
import functools

import jax
import jax.numpy as jnp
import numpy as np
from jax import lax
from jax.experimental import pallas as pl
from jax.experimental.pallas import tpu as pltpu
from jax.sharding import PartitionSpec as P

ROOT = 128
HALF = ROOT // 2
ROWS = 8


def split_np(table):
    table = table.astype(np.float32)
    high = table.astype(jnp.bfloat16)
    low = (table - high.astype(np.float32)).astype(jnp.bfloat16)
    return high, low


@functools.cache
def tables(tm_count):
    pos = np.arange(ROOT)
    short = 2.0 * np.pi * (np.outer(pos, pos) % ROOT) / ROOT
    cos_s, sin_s = np.cos(short), np.sin(short)
    first = np.concatenate([cos_s[:HALF], -sin_s[:HALF]], axis=0)
    first_hi, first_lo = split_np(first)
    first_all = np.concatenate(
        [
            np.concatenate([first_hi, first_hi], axis=1),
            np.concatenate([first_lo, first_lo], axis=1),
        ],
        axis=0,
    )
    bands = np.arange(HALF).reshape(tm_count, HALF // tm_count)
    order = np.concatenate([bands, ROOT - 1 - bands], axis=1).reshape(-1)
    cos_o, sin_o = cos_s[:, order], sin_s[:, order]
    second = np.concatenate(
        [np.concatenate([cos_o, -sin_o], axis=1), np.concatenate([sin_o, cos_o], axis=1)], axis=0
    )
    second_hi, second_lo = split_np(second)
    second_all = np.concatenate([second_hi, second_hi, second_lo], axis=0)
    long = 2.0 * np.pi * np.outer(np.arange(HALF + ROWS), pos) / (ROOT * ROOT)
    twist = np.concatenate([np.cos(long), np.sin(long)], axis=1).astype(np.float32)
    mirror = np.zeros((2 * ROOT, 2 * ROOT), np.float32)
    for side in range(2):
        for k in range(HALF):
            mirror[side * HALF + k, side * ROOT + k] = 1.0
            mirror[ROOT + side * HALF + k, side * ROOT + (ROOT - k if k else HALF)] = 1.0
    seg_len = ROOT * ROOT
    window = 0.5 - 0.5 * np.cos(2.0 * np.pi * np.arange(seg_len) / seg_len)
    energy = float(np.sum(window * window))
    return first_all, second_all, twist, window.reshape(ROOT, ROOT).astype(np.float32), mirror, energy


def split(value):
    high = value.astype(jnp.bfloat16)
    low = (value - high.astype(jnp.float32)).astype(jnp.bfloat16)
    return high, low


SPAN = 4
CORES = 2


RELAYED = (2, 4, 5)
RELAY_AT = (2, 6, 8)


def half_sum(ref):
    parts = [ref[:, ROOT * a : ROOT * (a + 1)] for a in range(HALF)]
    while len(parts) > 1:
        parts = [parts[n] + parts[n + 1] for n in range(0, len(parts), 2)]
    return jnp.sum(parts[0], axis=1, keepdims=True)


def stage_one(piece, mean, consts, buf, zbuf, ebuf, seg, segs):
    window_ref, first_ref, _, twist_ref = consts
    mean = jnp.broadcast_to(mean, (ROWS, ROOT))
    even = jnp.zeros((ROWS, ROOT), jnp.float32)
    odd = jnp.zeros((ROWS, ROOT), jnp.float32)
    for a in range(ROOT):
        tile = (piece[:, ROOT * a : ROOT * (a + 1)] - mean) * window_ref[a : a + 1, :]
        buf[ROWS * a : ROWS * (a + 1), :] = tile
        if a % 2 == 0:
            even = even + tile
        else:
            odd = odd + tile
    alt = even - odd
    sign = (1 - 2 * (lax.broadcasted_iota(jnp.int32, (ROWS, ROOT), 1) % 2)).astype(jnp.float32)
    edge = jnp.sum((even + odd) * sign, axis=1, keepdims=True)
    turn = twist_ref[HALF : HALF + 1, :]
    high, low = split(jnp.concatenate([alt * turn[:, :ROOT], -alt * turn[:, ROOT:]], axis=1))
    ebuf[seg * ROWS : (seg + 1) * ROWS, :] = jnp.concatenate([high, low, high], axis=1)
    cos_t, sin_t = twist_ref[:HALF, :ROOT], twist_ref[:HALF, ROOT:]
    for r in range(0, ROWS, 2):
        pair = jnp.concatenate(
            [buf[pl.ds(r, ROOT, stride=ROWS), :], buf[pl.ds(r + 1, ROOT, stride=ROWS), :]], axis=1
        )
        high, low = split(pair)
        out = jnp.dot(
            first_ref[...], jnp.concatenate([high, low], axis=0), preferred_element_type=jnp.float32
        )
        out = out[:ROOT] + out[ROOT:]
        for s in range(2):
            re = out[:HALF, s * ROOT : (s + 1) * ROOT]
            im = out[HALF:, s * ROOT : (s + 1) * ROOT]
            z_hi, z_lo = split(
                jnp.concatenate([re * cos_t + im * sin_t, im * cos_t - re * sin_t], axis=1)
            )
            at = ((r + s) * segs + seg) * HALF
            zbuf[at : at + HALF, 0 : 2 * ROOT] = z_hi
            zbuf[at : at + HALF, 2 * ROOT :] = z_lo
    return edge * edge


def squares(left, right):
    out = jnp.dot(left, right, preferred_element_type=jnp.float32)
    return out[:, :ROOT] * out[:, :ROOT] + out[:, ROOT:] * out[:, ROOT:]


def group_sums(side, rows, on, wait_halo, consts, scratch):
    second_ref = consts[2]
    buf, zbuf, ebuf, psum = scratch
    half_len = ROOT * HALF
    segs = 2 * CORES
    lane = lax.broadcasted_iota(jnp.int32, (ROWS, ROOT), 1)

    def window(start, length):
        return rows.at[:, pl.ds(pl.multiple_of(start, half_len), length)]

    own = side * half_len
    totals = [half_sum(window(own + h * half_len, half_len)) for h in range(segs)]
    inverse = 1.0 / (2 * half_len)
    nyq = jnp.zeros((ROWS, 1), jnp.float32)
    for seg in range(segs - 1):
        nyq = nyq + stage_one(
            window(own + seg * half_len, 2 * half_len), (totals[seg] + totals[seg + 1]) * inverse,
            consts, buf, zbuf, ebuf, seg, segs,
        )
    wait_halo()
    near = jnp.where(side == 0, totals[-1], totals[0])
    far = half_sum(window((1 - side) * segs * half_len, half_len))
    nyq = nyq + on * stage_one(
        window((1 - side) * (segs - 1) * half_len, 2 * half_len), (near + far) * inverse,
        consts, buf, zbuf, ebuf, segs - 1, segs,
    )

    def fold(power, count):
        total = power[:count]
        for seg in range(1, segs - 1):
            total = total + power[seg * count : (seg + 1) * count]
        return total + on * power[(segs - 1) * count :]

    for r in range(ROWS):
        at = slice(r * segs * HALF, (r + 1) * segs * HALF)
        left = jnp.concatenate([zbuf[at, :], zbuf[at, : 2 * ROOT]], axis=1)
        psum[r * HALF : (r + 1) * HALF, :] = fold(squares(left, second_ref[...]), HALF)
    mixed = fold(squares(ebuf[...], second_ref[...]), ROWS)
    first_rows = pl.ds(0, ROWS, stride=HALF)
    psum[first_rows, :] = jnp.where(lane % SPAN >= SPAN // 2, mixed, psum[first_rows, :])
    return nyq


def welch_kernel(
    scale, strain_ref, window_ref, first_ref, second_ref, twist_ref, mirror_ref,
    power_ref, nyquist_ref, mean_ref,
    data, relay_box, sums, fin, from_partner, z_in, x_in, nyq_rows, nyq_out, nyq_in, nyq_partner,
    buf, zbuf, ebuf, psum, mean_out, mean_in,
    load_sem, swap_send, swap_recv, halo_send, halo_recv, relay_send, relay_recv,
    z_send, z_recv, x_send, x_recv, core_send, core_recv,
    nyq_send, nyq_recv, nyq_core_send, nyq_core_recv, mean_send, mean_recv,
):
    chan, chan_count = lax.axis_index("chan"), lax.axis_size("chan")
    me = lax.axis_index("tm")
    core = lax.rem(me, CORES)
    chip = me // CORES
    chips = lax.axis_size("tm") // CORES
    z, x = chip // SPAN, lax.rem(chip, SPAN)
    half_len = ROOT * HALF
    block_len = 2 * half_len
    mine = data.shape[0]
    groups = mine // ROWS
    tile = ROWS // 2
    batches = groups // 2
    has_left, has_right = chip > 0, chip < chips - 1
    exists = (has_right, has_left)

    def as_int(flag):
        return flag.astype(jnp.int32)

    def device(chip_index, core_index):
        return {"tm": chip_index * CORES + core_index}

    def z_peer(step):
        return device(lax.rem(z + step + SPAN, SPAN) * SPAN + x, core)

    def x_peer(step):
        return device(z * SPAN + lax.rem(x + step + SPAN, SPAN), core)

    partner = device(chip, 1 - core)
    toward = 2 * core - 1
    sends_halo = jnp.where(core == 0, as_int(has_left), as_int(has_right)) == 1
    at_column = jnp.logical_or(x == 0, x == SPAN - 1)
    has_next_row = jnp.where(core == 0, as_int(z > 0), as_int(z < SPAN - 1)) == 1
    linked = jnp.logical_and(at_column, has_next_row)
    crosses = jnp.logical_and(linked, x == (SPAN - 1) * core)
    relays = jnp.logical_and(linked, x == (SPAN - 1) * (1 - core))
    faces = x == (SPAN - 1) * (1 - core)
    next_row = device(chip + toward * SPAN, 1 - core)

    def across(core_index):
        return device(z * SPAN + (SPAN - 1) - x, core_index)

    def remote(source, target, send, recv, where):
        return pltpu.make_async_remote_copy(
            src_ref=source, dst_ref=target, send_sem=send, recv_sem=recv,
            device_id=where, device_id_type=pl.DeviceIdType.MESH,
        )

    def strip(g):
        return pl.ds(pl.multiple_of(g * ROWS, ROWS), ROWS)

    def columns(g):
        start = lax.rem(g, 2) * half_len + core * block_len
        return pl.ds(pl.multiple_of(start, half_len), block_len)

    def load(g):
        rows = pl.ds(pl.multiple_of(core * mine + g * ROWS, ROWS), ROWS)
        return pltpu.make_async_copy(strain_ref.at[rows], data.at[strip(g), columns(g)], load_sem.at[g])

    def swap(g):
        rows = pl.ds(pl.multiple_of((1 - core) * mine + g * ROWS, ROWS), ROWS)
        return remote(
            strain_ref.at[rows], data.at[strip(g), columns(g)], swap_send.at[g], swap_recv.at[g], partner
        )

    def halo_place(n, side):
        start = (1 - side) * 2 * CORES * half_len
        return data.at[strip(2 * n + side), pl.ds(pl.multiple_of(start, half_len), half_len)]

    def halo_source(n, to):
        return strain_ref.at[
            pl.ds(pl.multiple_of(to * mine + (2 * n + core) * ROWS, ROWS), ROWS),
            pl.ds(pl.multiple_of(core * half_len, half_len), half_len),
        ]

    def halo_copy(n, to):
        return remote(
            halo_source(n, to), halo_place(n, core), halo_send.at[to, n], halo_recv.at[core, n],
            device(chip + toward, to),
        )

    def relay_copy(k, to):
        n = RELAYED[k]
        return remote(
            halo_source(n, to), relay_box.at[k, to], halo_send.at[to, n], relay_recv.at[k, to], next_row
        )

    def relay_on(k, to):
        n = RELAYED[k]
        return remote(
            relay_box.at[k, to], halo_place(n, 1 - core), relay_send.at[k, to],
            halo_recv.at[1 - core, n], across(to),
        )

    def halo_arrival(n, side):
        block = halo_place(n, side)
        return remote(block, block, halo_send.at[0, n], halo_recv.at[side, n], partner)

    @pl.loop(0, groups)
    def _(g):
        load(g).start()

    barrier = pltpu.get_barrier_semaphore()

    def greet(where):
        pl.semaphore_signal(barrier, inc=1, device_id=where, device_id_type=pl.DeviceIdType.MESH)

    def mean_peer(other, k):
        where = {"chan": lax.rem(chan + k, chan_count)}
        if other:
            where["tm"] = chip * CORES + 1 - core
        return where

    greet(partner)
    for k in range(1, SPAN):
        greet(z_peer(k))
        greet(x_peer(k))
    for k in range(1, chan_count):
        for other in range(2):
            greet(mean_peer(other, k))
    for flag, shift, both in ((has_left, -1, 0), (has_right, 1, 1)):
        @pl.when(flag)
        def _():
            greet(device(chip + shift, 1 - both))

            @pl.when(core == both)
            def _():
                greet(device(chip + shift, both))

    @pl.when(linked)
    def _():
        greet(next_row)

    @pl.when(faces)
    def _():
        greet(across(1 - core))

    left_count = as_int(has_left) * (2 - core)
    right_count = as_int(has_right) * (1 + core)
    pl.semaphore_wait(
        barrier,
        left_count + right_count + as_int(linked) + as_int(faces) + 1 + 2 * (SPAN - 1) + 2 * (chan_count - 1),
    )

    for n in range(batches):
        for side in range(2):
            swap(2 * n + side).start()

        @pl.when(sends_halo)
        def _():
            for to in range(CORES):
                if n in RELAYED:
                    @pl.when(crosses)
                    def _():
                        relay_copy(RELAYED.index(n), to).start()

                    @pl.when(jnp.logical_not(crosses))
                    def _():
                        halo_copy(n, to).start()
                else:
                    halo_copy(n, to).start()

    nyq_rows[...] = jnp.zeros_like(nyq_rows)
    consts = (window_ref, first_ref, second_ref, twist_ref)
    scratch = (buf, zbuf, ebuf, psum)

    def slab(i, size):
        return pl.ds(pl.multiple_of(i * size, size), size)

    def way(i):
        return 1 - 2 * lax.rem(i, 2)

    def z_block(i, step):
        return sums.at[slab(i, tile), lax.rem(z + step + SPAN, SPAN)]

    def x_block(i, step):
        return sums.at[slab(i, ROWS), z, lax.rem(x + step + SPAN, SPAN)]

    def ring(kind, i, block, inbox, send, recv, peer):
        d = way(i)
        step, hop = ((2, d), (-d, -d), (d, d))[kind]
        return remote(block(i, step), inbox.at[kind, i], send.at[kind, i], recv.at[kind, i], peer(hop))

    def z_copy(kind, i):
        return ring(kind, i, z_block, z_in, z_send, z_recv, z_peer)

    def x_copy(kind, i):
        return ring(kind, i, x_block, x_in, x_send, x_recv, x_peer)

    def core_copy(i):
        rows = slab(i, ROWS * ROWS)
        return remote(fin.at[rows], from_partner.at[rows], core_send.at[i], core_recv.at[i], partner)

    def begin(copy, i):
        copy(0, i).start()
        copy(1, i).start()

    def advance(copy, block, inbox, i):
        copy(0, i).wait_recv()
        target = block(i, way(i))
        target[...] = target[...] + inbox[0, i]
        copy(2, i).start()

    def collect(copy, block, inbox, i):
        copy(1, i).wait_recv()
        copy(2, i).wait_recv()
        return block(i, 0)[...] + inbox[1, i] + inbox[2, i]

    def z_advance(i):
        advance(z_copy, z_block, z_in, i)

    def z_collect(i):
        z_block(i, 0)[...] = collect(z_copy, z_block, z_in, i)

    def x_advance(i):
        advance(x_copy, x_block, x_in, i)

    def x_collect(i):
        fin[slab(i, ROWS * ROWS), :] = collect(x_copy, x_block, x_in, i).reshape(ROWS * ROWS, ROOT)
        core_copy(i).start()

    def nyq_copy(level, k):
        where = (z_peer, x_peer)[level](k)
        return remote(nyq_out.at[level], nyq_in.at[level, k], nyq_send.at[level, k], nyq_recv.at[level, k], where)

    def nyq_begin(level):
        nyq_in[level, 0] = nyq_out[level]
        for k in range(1, SPAN):
            nyq_copy(level, k).start()

    def nyq_collect(level):
        for k in range(1, SPAN):
            nyq_copy(level, k).wait_recv()
        here = (z, x)[level]
        total = nyq_in[level, lax.rem(here + SPAN, SPAN)]
        for source in range(1, SPAN):
            total = total + nyq_in[level, lax.rem(here - source + SPAN, SPAN)]
        nyq_out[level + 1] = total

    def nyq_final():
        return remote(nyq_out.at[2], nyq_partner, nyq_core_send, nyq_core_recv, partner)

    @pl.loop(0, groups)
    def _(t):
        side = lax.rem(t, 2)
        here = jnp.where(side == 0, as_int(has_right), as_int(has_left))
        load(t).wait()
        swap(t).wait_recv()

        for k in range(len(RELAYED)):
            @pl.when(jnp.logical_and(relays, t == RELAY_AT[k]))
            def _():
                for to in range(CORES):
                    relay_copy(k, to).wait_recv()
                    relay_on(k, to).start()

        def wait_halo():
            @pl.when(here == 1)
            def _():
                halo_arrival(t // 2, side).wait_recv()

            @pl.when(here == 0)
            def _():
                place = halo_place(t // 2, side)
                place[...] = jnp.zeros((ROWS, half_len), jnp.float32)

        nyq = group_sums(side, data.at[strip(t)], here.astype(jnp.float32), wait_halo, consts, scratch)
        nyq_rows[strip(t), :] = jnp.broadcast_to(nyq, (ROWS, ROOT))
        for p in range(tile):
            turned = jnp.transpose(psum[p * ROOT : (p + 1) * ROOT, :])
            sums[t * tile + p] = turned.reshape(sums.shape[1:])
        begin(z_copy, t)

        @pl.when(t >= 2)
        def _():
            z_advance(t - 2)

        @pl.when(t >= 4)
        def _():
            z_collect(t - 4)

    turned = jnp.transpose(nyq_rows[...])
    nyq_out[0] = turned[:ROWS]
    nyq_begin(0)
    early = batches - 2
    for b in range(early):
        begin(x_copy, b)
    z_advance(groups - 2)
    z_collect(groups - 4)
    z_collect(groups - 3)
    begin(x_copy, early)
    for b in range(early):
        x_advance(b)
    z_advance(groups - 1)
    nyq_collect(0)
    nyq_begin(1)
    x_advance(early)
    for b in range(early):
        x_collect(b)
    z_collect(groups - 2)
    z_collect(groups - 1)
    begin(x_copy, early + 1)
    nyq_collect(1)
    nyq_final().start()
    x_collect(early)
    x_advance(early + 1)
    x_collect(early + 1)

    lines = [fin[slab(i, ROWS), :] for i in range(fin.shape[0] // ROWS)]
    while len(lines) > 1:
        lines = [a + b for a, b in zip(lines[::2], lines[1::2])] + lines[len(lines) // 2 * 2 :]
    mean_out[...] = lines[0]

    def mean_copy(other, k):
        return remote(
            mean_out, mean_in.at[other, k], mean_send.at[other, k], mean_recv.at[other, k], mean_peer(other, k)
        )

    mean_links = [(other, k) for other in range(2) for k in range(chan_count) if other + k > 0]
    for link in mean_links:
        mean_copy(*link).start()
    mean_in[0, 0] = mean_out[...]

    nyq_final().wait_recv()
    for source in range(CORES):
        row = jnp.where(core == source, nyq_out[2], nyq_partner[...])
        nyquist_ref[source : source + 1, :] = row[:1] * scale

    lanes = lax.broadcasted_iota(jnp.int32, (1, ROOT), 1)

    def unfold(both):
        return jnp.dot(
            both, mirror_ref[...], precision=lax.Precision.HIGHEST, preferred_element_type=jnp.float32
        )

    factors = [jnp.where(jnp.logical_and(lanes == 0, me + j == 0), scale, 2.0 * scale) for j in range(2)]
    pairs = mine // 2
    for which, block in enumerate((fin, from_partner)):
        if which == 1:
            for b in range(batches):
                core_copy(b).wait_recv()
        base = (core if which == 0 else 1 - core) * mine
        for j in range(2):
            both = jnp.concatenate(
                [block[pl.ds(SPAN * core + j + shift, pairs, stride=ROWS), :] for shift in (0, 2)], axis=1
            )
            placed = unfold(both)
            for half in range(2):
                power_ref[pl.ds(j * CORES * mine + base + half, pairs, stride=2), :] = (
                    placed[:, half * ROOT : (half + 1) * ROOT] * factors[j]
                )

    for n in range(batches):
        for side in range(2):
            swap(2 * n + side).wait_send()
        core_copy(n).wait_send()

        @pl.when(sends_halo)
        def _():
            for to in range(CORES):
                halo_copy(n, to).wait_send()

        for kind in range(3):
            x_copy(kind, n).wait_send()

    @pl.loop(0, groups)
    def _(g):
        for kind in range(3):
            z_copy(kind, g).wait_send()

    @pl.when(relays)
    def _():
        for k in range(len(RELAYED)):
            for to in range(CORES):
                relay_on(k, to).wait_send()

    for level in range(2):
        for k in range(1, SPAN):
            nyq_copy(level, k).wait_send()
    nyq_final().wait_send()

    for link in mean_links:
        mean_copy(*link).wait()
    total = jnp.zeros((ROWS, ROOT), jnp.float32)
    for source_chan in range(chan_count):
        for source_core in range(CORES):
            total = total + mean_in[
                lax.rem(core + source_core, CORES), lax.rem(chan - source_chan + chan_count, chan_count)
            ]
    mean_out[...] = total
    rows = [mean_out[pl.ds(SPAN * core + j, 1), :] for j in range(SPAN)]
    placed = unfold(
        jnp.concatenate(
            [jnp.concatenate([rows[j], rows[j + 2]], axis=1) for j in range(2)]
            + [jnp.zeros((ROWS - 2, 2 * ROOT), jnp.float32)],
            axis=0,
        )
    )
    placed = placed[:, :ROOT] + placed[:, ROOT:]
    for j in range(2):
        mean_ref[j : j + 1, :] = placed[j : j + 1] * (factors[j] * (1.0 / (CORES * mine * chan_count)))


def per_device(strain):
    chan_rows, time_width = strain.shape
    seg_len = ROOT * ROOT
    half_len = seg_len // 2
    tm_count = lax.axis_size("tm")
    mine = chan_rows // CORES
    assert time_width == seg_len and tm_count == SPAN * SPAN * CORES and mine == 12 * ROWS
    segments = 2 * tm_count - 1
    first_all, second_all, twist, window, mirror, energy = tables(tm_count)
    pairs = mine // 2
    groups = mine // ROWS
    batches = groups // 2
    tile = ROWS // 2
    chan_count = lax.axis_size("chan")
    vmem = pl.BlockSpec(memory_space=pltpu.VMEM)
    f32 = jnp.float32
    dma = pltpu.SemaphoreType.DMA
    relayed = len(RELAYED)
    power, nyquist, mean_power = pl.pallas_call(
        functools.partial(welch_kernel, 1.0 / (segments * energy)),
        in_specs=[pl.BlockSpec(memory_space=pl.ANY)] + [vmem] * 5,
        out_specs=[vmem] * 3,
        out_shape=[
            jax.ShapeDtypeStruct((2 * chan_rows, ROOT), f32),
            jax.ShapeDtypeStruct((CORES, ROOT), f32),
            jax.ShapeDtypeStruct((2, ROOT), f32),
        ],
        scratch_shapes=[
            pltpu.VMEM((mine, CORES * seg_len + half_len), f32),
            pltpu.VMEM((relayed, CORES, ROWS, half_len), f32),
            pltpu.VMEM((pairs, SPAN, SPAN, ROWS, ROOT), f32),
            pltpu.VMEM((pairs * ROWS, ROOT), f32),
            pltpu.VMEM((pairs * ROWS, ROOT), f32),
            pltpu.VMEM((3, groups, tile, SPAN, ROWS, ROOT), f32),
            pltpu.VMEM((3, batches, ROWS, ROWS, ROOT), f32),
            pltpu.VMEM((ROOT, ROOT), f32),
            pltpu.VMEM((3, ROWS, ROOT), f32),
            pltpu.VMEM((2, SPAN, ROWS, ROOT), f32),
            pltpu.VMEM((ROWS, ROOT), f32),
            pltpu.VMEM((ROWS * ROOT, ROOT), f32),
            pltpu.VMEM((ROWS * 2 * CORES * HALF, 4 * ROOT), jnp.bfloat16),
            pltpu.VMEM((2 * CORES * ROWS, 6 * ROOT), jnp.bfloat16),
            pltpu.VMEM((ROWS * HALF, ROOT), f32),
            pltpu.VMEM((ROWS, ROOT), f32),
            pltpu.VMEM((2, chan_count, ROWS, ROOT), f32),
            dma((groups,)),
            dma((groups,)),
            dma((groups,)),
            dma((CORES, batches)),
            dma((2, batches)),
            dma((relayed, CORES)),
            dma((relayed, CORES)),
            dma((3, groups)),
            dma((3, groups)),
            dma((3, batches)),
            dma((3, batches)),
            dma((batches,)),
            dma((batches,)),
            dma((2, SPAN)),
            dma((2, SPAN)),
            dma(()),
            dma(()),
            dma((2, chan_count)),
            dma((2, chan_count)),
        ],
        compiler_params=pltpu.CompilerParams(
            collective_id=0, has_side_effects=True, vmem_limit_bytes=60 * 2**20
        ),
        name="welch",
    )(strain, window, first_all, second_all, twist, mirror)
    power = jnp.concatenate([power[:chan_rows], power[chan_rows:]], axis=1)
    return (power, nyquist[:, :mine].reshape(-1), mean_power.reshape(-1))


def solution(mesh):
    in_specs = (P("chan", "tm"),)
    out_specs = (P("chan", "tm"), P("chan"), P("tm"))
    return jax.shard_map(
        per_device, mesh=mesh, in_specs=in_specs, out_specs=out_specs, check_vma=False
    )
```

```python
import functools

import jax
import jax.numpy as jnp
import numpy as np
from jax import lax
from jax.experimental import pallas as pl
from jax.experimental.pallas import tpu as pltpu
from jax.sharding import PartitionSpec as P

ROOT = 128
HALF = ROOT // 2
ROWS = 8


def split_np(table):
    table = table.astype(np.float32)
    high = table.astype(jnp.bfloat16)
    low = (table - high.astype(np.float32)).astype(jnp.bfloat16)
    return high, low


@functools.cache
def tables(tm_count):
    pos = np.arange(ROOT)
    short = 2.0 * np.pi * (np.outer(pos, pos) % ROOT) / ROOT
    cos_s, sin_s = np.cos(short), np.sin(short)
    first = np.concatenate([cos_s[:HALF], -sin_s[:HALF]], axis=0)
    first_hi, first_lo = split_np(first)
    first_all = np.concatenate(
        [
            np.concatenate([first_hi, first_hi], axis=1),
            np.concatenate([first_lo, first_lo], axis=1),
        ],
        axis=0,
    )
    bands = np.arange(HALF).reshape(tm_count, HALF // tm_count)
    order = np.concatenate([bands, ROOT - 1 - bands], axis=1).reshape(-1)
    cos_o, sin_o = cos_s[:, order], sin_s[:, order]
    second = np.concatenate(
        [np.concatenate([cos_o, -sin_o], axis=1), np.concatenate([sin_o, cos_o], axis=1)], axis=0
    )
    second_hi, second_lo = split_np(second)
    second_all = np.concatenate([second_hi, second_hi, second_lo], axis=0)
    long = 2.0 * np.pi * np.outer(np.arange(HALF + ROWS), pos) / (ROOT * ROOT)
    twist = np.concatenate([np.cos(long), np.sin(long)], axis=1).astype(np.float32)
    mirror = np.zeros((2 * ROOT, 2 * ROOT), np.float32)
    for side in range(2):
        for k in range(HALF):
            mirror[side * HALF + k, side * ROOT + k] = 1.0
            mirror[ROOT + side * HALF + k, side * ROOT + (ROOT - k if k else HALF)] = 1.0
    seg_len = ROOT * ROOT
    window = 0.5 - 0.5 * np.cos(2.0 * np.pi * np.arange(seg_len) / seg_len)
    energy = float(np.sum(window * window))
    return first_all, second_all, twist, window.reshape(ROOT, ROOT).astype(np.float32), mirror.astype(jnp.bfloat16), energy


def split(value):
    high = value.astype(jnp.bfloat16)
    low = (value - high.astype(jnp.float32)).astype(jnp.bfloat16)
    return high, low


SPAN = 4
CORES = 2


RELAYED = (2, 4, 5)
RELAY_AT = (2, 5, 7)
HELD = 3
RING_AT = (3, 7)
X_START = ((9, 0, 4), (10, 4, 6), (11, 6, 8))


def half_sum(ref):
    parts = [ref[:, ROOT * a : ROOT * (a + 1)] for a in range(HALF)]
    while len(parts) > 1:
        parts = [parts[n] + parts[n + 1] for n in range(0, len(parts), 2)]
    return jnp.sum(parts[0], axis=1, keepdims=True)


def stage_one(piece, mean, consts, buf, zbuf, ebuf, seg, segs):
    window_ref, first_ref, _, twist_ref = consts
    mean = jnp.broadcast_to(mean, (ROWS, ROOT))
    even = jnp.zeros((ROWS, ROOT), jnp.float32)
    odd = jnp.zeros((ROWS, ROOT), jnp.float32)
    for a in range(ROOT):
        tile = (piece[:, ROOT * a : ROOT * (a + 1)] - mean) * window_ref[a : a + 1, :]
        buf[ROWS * a : ROWS * (a + 1), :] = tile
        if a % 2 == 0:
            even = even + tile
        else:
            odd = odd + tile
    alt = even - odd
    sign = (1 - 2 * (lax.broadcasted_iota(jnp.int32, (ROWS, ROOT), 1) % 2)).astype(jnp.float32)
    edge = jnp.sum((even + odd) * sign, axis=1, keepdims=True)
    turn = twist_ref[HALF : HALF + 1, :]
    high, low = split(jnp.concatenate([alt * turn[:, :ROOT], -alt * turn[:, ROOT:]], axis=1))
    ebuf[seg * ROWS : (seg + 1) * ROWS, :] = jnp.concatenate([high, low, high], axis=1)
    cos_t, sin_t = twist_ref[:HALF, :ROOT], twist_ref[:HALF, ROOT:]
    for r in range(0, ROWS, 2):
        pair = jnp.concatenate(
            [buf[pl.ds(r, ROOT, stride=ROWS), :], buf[pl.ds(r + 1, ROOT, stride=ROWS), :]], axis=1
        )
        high, low = split(pair)
        out = jnp.dot(
            first_ref[...], jnp.concatenate([high, low], axis=0), preferred_element_type=jnp.float32
        )
        out = out[:ROOT] + out[ROOT:]
        for s in range(2):
            re = out[:HALF, s * ROOT : (s + 1) * ROOT]
            im = out[HALF:, s * ROOT : (s + 1) * ROOT]
            z_hi, z_lo = split(
                jnp.concatenate([re * cos_t + im * sin_t, im * cos_t - re * sin_t], axis=1)
            )
            at = ((r + s) * segs + seg) * HALF
            zbuf[at : at + HALF, 0 : 2 * ROOT] = z_hi
            zbuf[at : at + HALF, 2 * ROOT :] = z_lo
    return edge * edge


def squares(left, right):
    out = jnp.dot(left, right, preferred_element_type=jnp.float32)
    return out[:, :ROOT] * out[:, :ROOT] + out[:, ROOT:] * out[:, ROOT:]


def group_sums(side, rows, on, wait_halo, consts, scratch):
    second_ref = consts[2]
    buf, zbuf, ebuf, psum = scratch
    half_len = ROOT * HALF
    segs = 2 * CORES
    lane = lax.broadcasted_iota(jnp.int32, (ROWS, ROOT), 1)

    def window(start, length):
        return rows.at[:, pl.ds(pl.multiple_of(start, half_len), length)]

    own = side * half_len
    totals = [half_sum(window(own + h * half_len, half_len)) for h in range(segs)]
    inverse = 1.0 / (2 * half_len)
    nyq = jnp.zeros((ROWS, 1), jnp.float32)
    for seg in range(segs - 1):
        nyq = nyq + stage_one(
            window(own + seg * half_len, 2 * half_len), (totals[seg] + totals[seg + 1]) * inverse,
            consts, buf, zbuf, ebuf, seg, segs,
        )
    wait_halo()
    near = jnp.where(side == 0, totals[-1], totals[0])
    far = half_sum(window((1 - side) * segs * half_len, half_len))
    nyq = nyq + on * stage_one(
        window((1 - side) * (segs - 1) * half_len, 2 * half_len), (near + far) * inverse,
        consts, buf, zbuf, ebuf, segs - 1, segs,
    )

    def fold(power, count):
        total = power[:count]
        for seg in range(1, segs - 1):
            total = total + power[seg * count : (seg + 1) * count]
        return total + on * power[(segs - 1) * count :]

    for r in range(ROWS):
        at = slice(r * segs * HALF, (r + 1) * segs * HALF)
        left = jnp.concatenate([zbuf[at, :], zbuf[at, : 2 * ROOT]], axis=1)
        psum[r * HALF : (r + 1) * HALF, :] = fold(squares(left, second_ref[...]), HALF)
    mixed = fold(squares(ebuf[...], second_ref[...]), ROWS)
    first_rows = pl.ds(0, ROWS, stride=HALF)
    psum[first_rows, :] = jnp.where(lane % SPAN >= SPAN // 2, mixed, psum[first_rows, :])
    return nyq


def welch_kernel(
    scale, strain_ref, window_hbm, first_hbm, second_hbm, twist_hbm, mirror_hbm, packed_ref,
    window_ref, first_ref, second_ref, twist_ref, mirror_ref, power_box, small_box, table_sem, out_sem,
    data, relay_box, sums, fin, from_partner, z_in, x_in, direct_in, nyq_box, nyq_rows,
    buf, zbuf, ebuf, psum, mean_out, mean_in,
    load_sem, swap_send, swap_recv, halo_send, halo_recv, relay_send, relay_recv,
    z_send, z_recv, x_send, x_recv, direct_send, direct_recv, core_send, core_recv, mean_send, mean_recv,
):
    chan, chan_count = lax.axis_index("chan"), lax.axis_size("chan")
    me = lax.axis_index("tm")
    core = lax.rem(me, CORES)
    chip = me // CORES
    chips = lax.axis_size("tm") // CORES
    z, x = chip // SPAN, lax.rem(chip, SPAN)
    half_len = ROOT * HALF
    block_len = 2 * half_len
    mine = data.shape[0]
    groups = mine // ROWS
    tile = ROWS // 2
    batches = groups // 2
    ringed = groups
    size = tile * ROWS
    ring_at = jnp.where(jnp.logical_or(x == 0, x == SPAN - 1), RING_AT[1], RING_AT[0])
    has_left, has_right = chip > 0, chip < chips - 1
    exists = (has_right, has_left)

    def as_int(flag):
        return flag.astype(jnp.int32)

    def device(chip_index, core_index):
        return {"tm": chip_index * CORES + core_index}

    def z_peer(step):
        return device(lax.rem(z + step + SPAN, SPAN) * SPAN + x, core)

    def x_peer(step):
        return device(z * SPAN + lax.rem(x + step + SPAN, SPAN), core)

    partner = device(chip, 1 - core)
    toward = 2 * core - 1
    sends_halo = jnp.where(core == 0, as_int(has_left), as_int(has_right)) == 1
    at_column = jnp.logical_or(x == 0, x == SPAN - 1)
    has_next_row = jnp.where(core == 0, as_int(z > 0), as_int(z < SPAN - 1)) == 1
    linked = jnp.logical_and(at_column, has_next_row)
    crosses = jnp.logical_and(linked, x == (SPAN - 1) * core)
    relays = jnp.logical_and(linked, x == (SPAN - 1) * (1 - core))
    faces = x == (SPAN - 1) * (1 - core)
    next_row = device(chip + toward * SPAN, 1 - core)

    def across(core_index):
        return device(z * SPAN + (SPAN - 1) - x, core_index)

    def remote(source, target, send, recv, where):
        return pltpu.make_async_remote_copy(
            src_ref=source, dst_ref=target, send_sem=send, recv_sem=recv,
            device_id=where, device_id_type=pl.DeviceIdType.MESH,
        )

    def strip(g):
        return pl.ds(pl.multiple_of(g * ROWS, ROWS), ROWS)

    def columns(g, side):
        start = side * half_len + core * block_len
        return pl.ds(pl.multiple_of(start, half_len), block_len)

    def load(g):
        rows = pl.ds(pl.multiple_of(core * mine + g * ROWS, ROWS), ROWS)
        place = data.at[strip(g), columns(g, lax.rem(g + core, 2))]
        return pltpu.make_async_copy(strain_ref.at[rows], place, load_sem.at[g])

    def swap(g):
        rows = pl.ds(pl.multiple_of((1 - core) * mine + g * ROWS, ROWS), ROWS)
        place = data.at[strip(g), columns(g, lax.rem(g + 1 - core, 2))]
        return remote(strain_ref.at[rows], place, swap_send, swap_recv.at[g], partner)

    def halo_group(n, side, to):
        return 2 * n + lax.rem(side + to, 2)

    def halo_place(n, side, to):
        start = (1 - side) * 2 * CORES * half_len
        return data.at[strip(halo_group(n, side, to)), pl.ds(pl.multiple_of(start, half_len), half_len)]

    def halo_source(n, to):
        return strain_ref.at[
            pl.ds(pl.multiple_of(to * mine + halo_group(n, core, to) * ROWS, ROWS), ROWS),
            pl.ds(pl.multiple_of(core * half_len, half_len), half_len),
        ]

    def halo_copy(n, to):
        return remote(
            halo_source(n, to), halo_place(n, core, to), halo_send, halo_recv.at[core, n],
            device(chip + toward, to),
        )

    def relay_copy(k, to):
        n = RELAYED[k]
        return remote(
            halo_source(n, to), relay_box.at[k, to], halo_send, relay_recv.at[k, to], next_row
        )

    def relay_on(k, to):
        n = RELAYED[k]
        return remote(
            relay_box.at[k, to], halo_place(n, 1 - core, to), relay_send,
            halo_recv.at[1 - core, n], across(to),
        )

    def halo_arrival(n, side):
        block = halo_place(n, side, core)
        return remote(block, block, halo_send, halo_recv.at[side, n], partner)

    barrier = pltpu.get_barrier_semaphore()

    def greet(where):
        pl.semaphore_signal(barrier, inc=1, device_id=where, device_id_type=pl.DeviceIdType.MESH)

    def mean_peer(other, k):
        where = {"chan": lax.rem(chan + k, chan_count)}
        if other:
            where["tm"] = chip * CORES + 1 - core
        return where

    def chip_peer(k):
        far_z, far_x = lax.rem(z + k // SPAN, SPAN), lax.rem(x + k % SPAN, SPAN)
        return far_z, far_x, device(far_z * SPAN + far_x, core)

    greet(partner)
    for k in range(1, SPAN * SPAN):
        greet(chip_peer(k)[2])
    for k in range(1, chan_count):
        for other in range(2):
            greet(mean_peer(other, k))
    for flag, shift, both in ((has_left, -1, 0), (has_right, 1, 1)):
        @pl.when(flag)
        def _():
            greet(device(chip + shift, 1 - both))

            @pl.when(core == both)
            def _():
                greet(device(chip + shift, both))

    @pl.when(linked)
    def _():
        greet(next_row)

    @pl.when(faces)
    def _():
        greet(across(1 - core))

    tables_in = [
        pltpu.make_async_copy(source, target, table_sem.at[n])
        for n, (source, target) in enumerate(
            zip(
                (window_hbm, first_hbm, second_hbm, twist_hbm, mirror_hbm),
                (window_ref, first_ref, second_ref, twist_ref, mirror_ref),
            )
        )
    ]
    load(0).start()
    for table in tables_in:
        table.start()

    @pl.loop(1, groups)
    def _(g):
        load(g).start()

    left_count = as_int(has_left) * (2 - core)
    right_count = as_int(has_right) * (1 + core)
    pl.semaphore_wait(
        barrier,
        left_count + right_count + as_int(linked) + as_int(faces) + SPAN * SPAN + 2 * (chan_count - 1),
    )

    for n in range(batches):
        for side in range(2):
            swap(2 * n + side).start()

        @pl.when(sends_halo)
        def _():
            for turn in range(CORES):
                to = lax.rem(core + turn, CORES)
                if n in RELAYED:
                    @pl.when(crosses)
                    def _():
                        relay_copy(RELAYED.index(n), to).start()

                    @pl.when(jnp.logical_not(crosses))
                    def _():
                        halo_copy(n, to).start()
                elif n == HELD:
                    @pl.when(jnp.logical_not(crosses))
                    def _():
                        halo_copy(n, to).start()
                else:
                    halo_copy(n, to).start()

    nyq_rows[...] = jnp.zeros_like(nyq_rows)
    for table in tables_in:
        table.wait()
    consts = (window_ref, first_ref, second_ref, twist_ref)
    scratch = (buf, zbuf, ebuf, psum)

    def slab(i, size):
        return pl.ds(pl.multiple_of(i * size, size), size)

    def way(i):
        return 1 - 2 * lax.rem(i, 2)

    def z_block(i, step):
        return sums.at[slab(i, tile), lax.rem(z + step + SPAN, SPAN)]

    def x_block(i, step):
        return sums.at[slab(i, tile), z, lax.rem(x + step + SPAN, SPAN)]

    def ring(kind, i, block, inbox, send, recv, peer):
        d = way(i)
        step, hop = ((2, d), (-d, -d), (d, d))[kind]
        return remote(block(i, step), inbox.at[kind, i], send, recv.at[kind, i], peer(hop))

    def z_copy(kind, i):
        return ring(kind, i, z_block, z_in, z_send, z_recv, z_peer)

    def x_copy(kind, i):
        return ring(kind, i, x_block, x_in, x_send, x_recv, x_peer)

    def core_copy(i):
        count = 2 * size + (ROWS if i == batches - 1 else 0)
        rows = pl.ds(i * 2 * size, count)
        return remote(fin.at[rows], from_partner.at[rows], core_send, core_recv.at[i], partner)

    def direct_copy(k):
        far_z, far_x, where = chip_peer(k)
        return remote(nyq_box, direct_in.at[k], direct_send, direct_recv, where)

    def direct_all():
        box = direct_in.at[pl.ds(1, SPAN * SPAN - 1)]
        return remote(box, box, direct_send, direct_recv, partner)

    def send_direct():
        for k in (10, 6, 9, 11, 14, 2, 8, 5, 7, 13, 15, 1, 3, 4, 12):
            direct_copy(k).start()

    def sum_direct():
        direct_all().wait_recv()
        nyq = jnp.zeros((ROWS, ROOT), jnp.float32)
        for far_z in range(SPAN):
            for far_x in range(SPAN):
                k = lax.rem(z - far_z + SPAN, SPAN) * SPAN + lax.rem(x - far_x + SPAN, SPAN)
                nyq = nyq + direct_in[k]
        fin[pl.ds(groups * size, ROWS), :] = nyq

    def begin(copy, i):
        copy(0, i).start()
        copy(1, i).start()

    def advance(copy, block, inbox, i):
        copy(0, i).wait_recv()
        target = block(i, way(i))
        target[...] = target[...] + inbox[0, i]
        copy(2, i).start()

    def collect(copy, block, inbox, i):
        copy(1, i).wait_recv()
        copy(2, i).wait_recv()
        return block(i, 0)[...] + inbox[1, i] + inbox[2, i]

    def z_advance(i):
        advance(z_copy, z_block, z_in, i)

    def z_collect(i):
        z_block(i, 0)[...] = collect(z_copy, z_block, z_in, i)

    def x_advance(i):
        advance(x_copy, x_block, x_in, i)

    def x_collect(i):
        rows = pl.ds(pl.multiple_of(i * size, size), size)
        fin[rows, :] = collect(x_copy, x_block, x_in, i).reshape(size, ROOT)

    @pl.loop(0, groups)
    def _(t):
        side = lax.rem(t + core, 2)
        here = jnp.where(side == 0, as_int(has_right), as_int(has_left))
        load(t).wait()
        swap(t).wait_recv()

        for k in range(len(RELAYED)):
            @pl.when(jnp.logical_and(relays, t == RELAY_AT[k]))
            def _():
                for turn in range(CORES):
                    to = lax.rem(1 - core + turn, CORES)
                    relay_copy(k, to).wait_recv()
                    relay_on(k, to).start()

        @pl.when(jnp.logical_and(crosses, t == HELD))
        def _():
            for turn in range(CORES):
                halo_copy(HELD, lax.rem(core + turn, CORES)).start()

        def wait_halo():
            @pl.when(t == ring_at)
            def _():
                @pl.loop(0, ring_at - 2)
                def _(i):
                    z_advance(i)

            @pl.when(t >= ring_at)
            def _():
                z_advance(t - 2)

            for at, first, last in X_START:
                @pl.when(t == at)
                def _():
                    @pl.loop(first, last)
                    def _(i):
                        z_collect(i)
                        begin(x_copy, i)

            @pl.when(t == groups - 1)
            def _():
                @pl.loop(0, 4)
                def _(i):
                    x_advance(i)

            @pl.when(here == 1)
            def _():
                halo_arrival(t // 2, side).wait_recv()

            @pl.when(here == 0)
            def _():
                place = halo_place(t // 2, side, core)
                place[...] = jnp.zeros((ROWS, half_len), jnp.float32)

        nyq = group_sums(side, data.at[strip(t)], here.astype(jnp.float32), wait_halo, consts, scratch)
        nyq_rows[strip(t), :] = jnp.broadcast_to(nyq, (ROWS, ROOT))
        for p in range(tile):
            turned = jnp.transpose(psum[p * ROOT : (p + 1) * ROOT, :])
            sums[t * tile + p] = turned.reshape(sums.shape[1:])

        begin(z_copy, t)

    nyq_box[...] = jnp.transpose(nyq_rows[...])[:ROWS]
    direct_in[0] = nyq_box[...]
    z_advance(10)
    send_direct()
    x_advance(4)
    x_advance(5)
    z_collect(8)
    begin(x_copy, 8)
    for i in range(4):
        x_collect(i)
    core_copy(0).start()
    core_copy(1).start()
    x_advance(6)
    x_advance(7)
    z_collect(9)
    begin(x_copy, 9)
    z_advance(11)
    x_collect(4)
    x_collect(5)
    core_copy(2).start()
    z_collect(10)
    begin(x_copy, 10)
    x_advance(8)
    x_collect(6)
    x_collect(7)
    core_copy(3).start()
    x_advance(9)
    z_collect(11)
    begin(x_copy, 11)
    x_advance(10)
    x_collect(8)
    x_collect(9)
    core_copy(4).start()
    x_advance(11)
    x_collect(10)
    sum_direct()
    x_collect(11)
    core_copy(5).start()

    lines = [fin[slab(i, ROWS), :] for i in range(groups * tile)]
    while len(lines) > 1:
        lines = [a + b for a, b in zip(lines[::2], lines[1::2])] + lines[len(lines) // 2 * 2 :]
    mean_out[...] = lines[0]

    def mean_copy(other, k):
        return remote(
            mean_out, mean_in.at[other, k], mean_send.at[other, k], mean_recv.at[other, k], mean_peer(other, k)
        )

    mean_links = [(other, k) for other in range(2) for k in range(chan_count) if other + k > 0]
    for link in mean_links:
        mean_copy(*link).start()
    mean_in[0, 0] = mean_out[...]

    lanes = lax.broadcasted_iota(jnp.int32, (1, ROOT), 1)

    def unfold(both):
        high = both.astype(jnp.bfloat16)
        middle = (both - high.astype(jnp.float32)).astype(jnp.bfloat16)
        rest = both - high.astype(jnp.float32) - middle.astype(jnp.float32)
        low = rest.astype(jnp.bfloat16)
        parts = [jnp.dot(part, mirror_ref[...], preferred_element_type=jnp.float32) for part in (low, middle, high)]
        return parts[0] + parts[1] + parts[2]

    factors = [jnp.where(jnp.logical_and(lanes == 0, me + j == 0), scale, 2.0 * scale) for j in range(2)]
    pairs = mine // 2
    for which, block in enumerate((fin, from_partner)):
        if which == 1:
            for b in range(batches):
                core_copy(b).wait_recv()
        base = (core if which == 0 else 1 - core) * mine
        for j in range(2):
            both = jnp.concatenate(
                [block[pl.ds(SPAN * core + j + shift, pairs, stride=ROWS), :] for shift in (0, 2)], axis=1
            )
            placed = unfold(both)
            for half in range(2):
                power_box[pl.ds(j * CORES * mine + base + half, pairs, stride=2), :] = (
                    placed[:, half * ROOT : (half + 1) * ROOT] * factors[j]
                )

    power_out = pltpu.make_async_copy(power_box, packed_ref.at[: power_box.shape[0]], out_sem.at[0])
    power_out.start()

    ends = [
        ref[groups * size : groups * size + 1, :] * scale for ref in (fin, from_partner)
    ]
    parts = [jnp.where(core == source, ends[0], ends[1]) for source in range(CORES)]
    moved = pltpu.roll(parts[1], mine, 1)
    small_box[...] = jnp.zeros_like(small_box)
    small_box[0:1, :] = jnp.where(lanes < mine, parts[0], moved)
    small_box[1:2, :] = moved

    def sent(box, send):
        remote(box, box, send, core_recv.at[0], partner).wait_send()

    sent(strain_ref.at[pl.ds(0, mine)], swap_send)
    sent(z_in, z_send)
    sent(x_in, x_send)
    sent(fin, core_send)
    direct_all().wait_send()

    @pl.when(sends_halo)
    def _():
        sent(strain_ref.at[pl.ds(0, mine), pl.ds(0, half_len)], halo_send)

    @pl.when(relays)
    def _():
        sent(relay_box, relay_send)

    for link in mean_links:
        mean_copy(*link).wait()
    total = jnp.zeros((ROWS, ROOT), jnp.float32)
    for source_chan in range(chan_count):
        for source_core in range(CORES):
            total = total + mean_in[
                lax.rem(core + source_core, CORES), lax.rem(chan - source_chan + chan_count, chan_count)
            ]
    mean_out[...] = total
    rows = [mean_out[pl.ds(SPAN * core + j, 1), :] for j in range(SPAN)]
    placed = unfold(
        jnp.concatenate(
            [jnp.concatenate([rows[j], rows[j + 2]], axis=1) for j in range(2)]
            + [jnp.zeros((ROWS - 2, 2 * ROOT), jnp.float32)],
            axis=0,
        )
    )
    placed = placed[:, :ROOT] + placed[:, ROOT:]
    for j in range(2):
        small_box[2 + j : 3 + j, :] = placed[j : j + 1] * (factors[j] * (1.0 / (CORES * mine * chan_count)))
    small_out = pltpu.make_async_copy(small_box, packed_ref.at[power_box.shape[0] :], out_sem.at[1])
    small_out.start()
    power_out.wait()
    small_out.wait()


def finish_kernel(packed_ref, power_ref, nyquist_ref, mean_ref):
    chan_rows = power_ref.shape[0]
    for j in range(2):
        power_ref[:, j * ROOT : (j + 1) * ROOT] = packed_ref[j * chan_rows : (j + 1) * chan_rows, :]
        mean_ref[:, j * ROOT : (j + 1) * ROOT] = packed_ref[2 * chan_rows + 2 + j : 2 * chan_rows + 3 + j, :]
    nyquist_ref[:, :ROOT] = packed_ref[2 * chan_rows : 2 * chan_rows + 1, :]
    nyquist_ref[:, ROOT:] = packed_ref[2 * chan_rows + 1 : 2 * chan_rows + 2, : chan_rows - ROOT]


def per_device(strain):
    chan_rows, time_width = strain.shape
    seg_len = ROOT * ROOT
    half_len = seg_len // 2
    tm_count = lax.axis_size("tm")
    mine = chan_rows // CORES
    assert time_width == seg_len and tm_count == SPAN * SPAN * CORES and mine == 12 * ROWS
    segments = 2 * tm_count - 1
    first_all, second_all, twist, window, mirror, energy = tables(tm_count)
    pairs = mine // 2
    groups = mine // ROWS
    batches = groups // 2
    tile = ROWS // 2
    chan_count = lax.axis_size("chan")
    vmem = pl.BlockSpec(memory_space=pltpu.VMEM)
    f32 = jnp.float32
    dma = pltpu.SemaphoreType.DMA
    relayed = len(RELAYED)
    tables_in = (window, first_all, second_all, twist, mirror)
    packed = pl.pallas_call(
        functools.partial(welch_kernel, 1.0 / (segments * energy)),
        in_specs=[pl.BlockSpec(memory_space=pl.ANY)] * 6,
        out_specs=pl.BlockSpec(memory_space=pl.ANY),
        out_shape=jax.ShapeDtypeStruct((2 * chan_rows + ROWS, ROOT), f32),
        scratch_shapes=[pltpu.VMEM(table.shape, table.dtype) for table in tables_in]
        + [
            pltpu.VMEM((2 * chan_rows, ROOT), f32),
            pltpu.VMEM((ROWS, ROOT), f32),
            dma((len(tables_in),)),
            dma((2,)),
            pltpu.VMEM((mine, CORES * seg_len + half_len), f32),
            pltpu.VMEM((relayed, CORES, ROWS, half_len), f32),
            pltpu.VMEM((pairs, SPAN, SPAN, ROWS, ROOT), f32),
            pltpu.VMEM(((pairs + 1) * ROWS, ROOT), f32),
            pltpu.VMEM(((pairs + 1) * ROWS, ROOT), f32),
            pltpu.VMEM((3, groups, tile, SPAN, ROWS, ROOT), f32),
            pltpu.VMEM((3, groups, tile, ROWS, ROOT), f32),
            pltpu.VMEM((SPAN * SPAN, ROWS, ROOT), f32),
            pltpu.VMEM((ROWS, ROOT), f32),
            pltpu.VMEM((ROOT, ROOT), f32),
            pltpu.VMEM((ROWS * ROOT, ROOT), f32),
            pltpu.VMEM((ROWS * 2 * CORES * HALF, 4 * ROOT), jnp.bfloat16),
            pltpu.VMEM((2 * CORES * ROWS, 6 * ROOT), jnp.bfloat16),
            pltpu.VMEM((ROWS * HALF, ROOT), f32),
            pltpu.VMEM((ROWS, ROOT), f32),
            pltpu.VMEM((2, chan_count, ROWS, ROOT), f32),
            dma((groups,)),
            dma(()),
            dma((groups,)),
            dma(()),
            dma((2, batches)),
            dma(()),
            dma((relayed, CORES)),
            dma(()),
            dma((3, groups)),
            dma(()),
            dma((3, groups)),
            dma(()),
            dma(()),
            dma(()),
            dma((batches,)),
            dma((2, chan_count)),
            dma((2, chan_count)),
        ],
        compiler_params=pltpu.CompilerParams(
            collective_id=0, has_side_effects=True, vmem_limit_bytes=60 * 2**20
        ),
        name="welch",
    )(strain, *tables_in)
    power, nyquist, mean_power = pl.pallas_call(
        finish_kernel,
        in_specs=[vmem],
        out_specs=[vmem] * 3,
        out_shape=[
            jax.ShapeDtypeStruct((chan_rows, 2 * ROOT), f32),
            jax.ShapeDtypeStruct((1, chan_rows), f32),
            jax.ShapeDtypeStruct((1, 2 * ROOT), f32),
        ],
        name="finish",
    )(packed)
    return (power, nyquist.reshape(-1), mean_power.reshape(-1))


def solution(mesh):
    in_specs = (P("chan", "tm"),)
    out_specs = (P("chan", "tm"), P("chan"), P("tm"))
    return jax.shard_map(
        per_device, mesh=mesh, in_specs=in_specs, out_specs=out_specs, check_vma=False
    )
```

```python
import functools

import jax
import jax.numpy as jnp
import numpy as np
from jax import lax
from jax.experimental import pallas as pl
from jax.experimental.pallas import tpu as pltpu
from jax.sharding import PartitionSpec as P

ROOT = 128
HALF = ROOT // 2
ROWS = 8


def split_np(table):
    table = table.astype(np.float32)
    high = table.astype(jnp.bfloat16)
    low = (table - high.astype(np.float32)).astype(jnp.bfloat16)
    return high, low


@functools.cache
def tables(tm_count):
    pos = np.arange(ROOT)
    short = 2.0 * np.pi * (np.outer(pos, pos) % ROOT) / ROOT
    cos_s, sin_s = np.cos(short), np.sin(short)
    first = np.concatenate([cos_s[:HALF], -sin_s[:HALF]], axis=0)
    first_hi, first_lo = split_np(first)
    first_all = np.concatenate(
        [
            np.concatenate([first_hi, first_hi], axis=1),
            np.concatenate([first_lo, first_lo], axis=1),
        ],
        axis=0,
    )
    bands = np.arange(HALF).reshape(tm_count, HALF // tm_count)
    order = np.concatenate([bands, ROOT - 1 - bands], axis=1).reshape(-1)
    cos_o, sin_o = cos_s[:, order], sin_s[:, order]
    second = np.concatenate(
        [np.concatenate([cos_o, -sin_o], axis=1), np.concatenate([sin_o, cos_o], axis=1)], axis=0
    )
    second_hi, second_lo = split_np(second)
    second_all = np.concatenate([second_hi, second_hi, second_lo], axis=0)
    long = 2.0 * np.pi * np.outer(np.arange(HALF + ROWS), pos) / (ROOT * ROOT)
    twist = np.concatenate([np.cos(long), np.sin(long)], axis=1).astype(np.float32)
    mirror = np.zeros((2 * ROOT, 2 * ROOT), np.float32)
    for side in range(2):
        for k in range(HALF):
            mirror[side * HALF + k, side * ROOT + k] = 1.0
            mirror[ROOT + side * HALF + k, side * ROOT + (ROOT - k if k else HALF)] = 1.0
    seg_len = ROOT * ROOT
    window = 0.5 - 0.5 * np.cos(2.0 * np.pi * np.arange(seg_len) / seg_len)
    energy = float(np.sum(window * window))
    return first_all, second_all, twist, window.reshape(ROOT, ROOT).astype(np.float32), mirror.astype(jnp.bfloat16), energy


def split(value):
    high = value.astype(jnp.bfloat16)
    low = (value - high.astype(jnp.float32)).astype(jnp.bfloat16)
    return high, low


SPAN = 4
CORES = 2


RELAYED = (2, 4, 5)
RELAY_AT = (2, 5, 7)
HELD = 3
LATE = ((7, 0, 4), (8, 4, 6), (9, 6, 8), (10, 8, 9), (11, 9, 10))
SHORT = 8
X_START = ((9, 0, 4), (10, 4, 6), (11, 6, 8))


def half_sum(ref):
    parts = [ref[:, ROOT * a : ROOT * (a + 1)] for a in range(HALF)]
    while len(parts) > 1:
        parts = [parts[n] + parts[n + 1] for n in range(0, len(parts), 2)]
    return jnp.sum(parts[0], axis=1, keepdims=True)


def stage_one(piece, mean, consts, buf, zbuf, ebuf, seg, segs):
    window_ref, first_ref, _, twist_ref = consts
    mean = jnp.broadcast_to(mean, (ROWS, ROOT))
    even = jnp.zeros((ROWS, ROOT), jnp.float32)
    odd = jnp.zeros((ROWS, ROOT), jnp.float32)
    for a in range(ROOT):
        tile = (piece[:, ROOT * a : ROOT * (a + 1)] - mean) * window_ref[a : a + 1, :]
        buf[ROWS * a : ROWS * (a + 1), :] = tile
        if a % 2 == 0:
            even = even + tile
        else:
            odd = odd + tile
    alt = even - odd
    sign = (1 - 2 * (lax.broadcasted_iota(jnp.int32, (ROWS, ROOT), 1) % 2)).astype(jnp.float32)
    edge = jnp.sum((even + odd) * sign, axis=1, keepdims=True)
    turn = twist_ref[HALF : HALF + 1, :]
    high, low = split(jnp.concatenate([alt * turn[:, :ROOT], -alt * turn[:, ROOT:]], axis=1))
    ebuf[seg * ROWS : (seg + 1) * ROWS, :] = jnp.concatenate([high, low, high], axis=1)
    cos_t, sin_t = twist_ref[:HALF, :ROOT], twist_ref[:HALF, ROOT:]
    for r in range(0, ROWS, 2):
        pair = jnp.concatenate(
            [buf[pl.ds(r, ROOT, stride=ROWS), :], buf[pl.ds(r + 1, ROOT, stride=ROWS), :]], axis=1
        )
        high, low = split(pair)
        out = jnp.dot(
            first_ref[...], jnp.concatenate([high, low], axis=0), preferred_element_type=jnp.float32
        )
        out = out[:ROOT] + out[ROOT:]
        for s in range(2):
            re = out[:HALF, s * ROOT : (s + 1) * ROOT]
            im = out[HALF:, s * ROOT : (s + 1) * ROOT]
            z_hi, z_lo = split(
                jnp.concatenate([re * cos_t + im * sin_t, im * cos_t - re * sin_t], axis=1)
            )
            at = ((r + s) * segs + seg) * HALF
            zbuf[at : at + HALF, 0 : 2 * ROOT] = z_hi
            zbuf[at : at + HALF, 2 * ROOT :] = z_lo
    return edge * edge


def squares(left, right):
    out = jnp.dot(left, right, preferred_element_type=jnp.float32)
    return out[:, :ROOT] * out[:, :ROOT] + out[:, ROOT:] * out[:, ROOT:]


def group_sums(side, rows, on, wait_halo, consts, scratch):
    second_ref = consts[2]
    buf, zbuf, ebuf, psum = scratch
    half_len = ROOT * HALF
    segs = 2 * CORES
    lane = lax.broadcasted_iota(jnp.int32, (ROWS, ROOT), 1)

    def window(start, length):
        return rows.at[:, pl.ds(pl.multiple_of(start, half_len), length)]

    own = side * half_len
    totals = [half_sum(window(own + h * half_len, half_len)) for h in range(segs)]
    inverse = 1.0 / (2 * half_len)
    nyq = jnp.zeros((ROWS, 1), jnp.float32)
    for seg in range(segs - 1):
        nyq = nyq + stage_one(
            window(own + seg * half_len, 2 * half_len), (totals[seg] + totals[seg + 1]) * inverse,
            consts, buf, zbuf, ebuf, seg, segs,
        )
    wait_halo()
    near = jnp.where(side == 0, totals[-1], totals[0])
    far = half_sum(window((1 - side) * segs * half_len, half_len))
    nyq = nyq + on * stage_one(
        window((1 - side) * (segs - 1) * half_len, 2 * half_len), (near + far) * inverse,
        consts, buf, zbuf, ebuf, segs - 1, segs,
    )

    def fold(power, count):
        total = power[:count]
        for seg in range(1, segs - 1):
            total = total + power[seg * count : (seg + 1) * count]
        return total + on * power[(segs - 1) * count :]

    for r in range(ROWS):
        at = slice(r * segs * HALF, (r + 1) * segs * HALF)
        left = jnp.concatenate([zbuf[at, :], zbuf[at, : 2 * ROOT]], axis=1)
        psum[r * HALF : (r + 1) * HALF, :] = fold(squares(left, second_ref[...]), HALF)
    mixed = fold(squares(ebuf[...], second_ref[...]), ROWS)
    first_rows = pl.ds(0, ROWS, stride=HALF)
    psum[first_rows, :] = jnp.where(lane % SPAN >= SPAN // 2, mixed, psum[first_rows, :])
    return nyq


def welch_kernel(
    scale, strain_ref, window_hbm, first_hbm, second_hbm, twist_hbm, mirror_hbm, packed_ref,
    window_ref, first_ref, second_ref, twist_ref, mirror_ref, power_box, small_box, table_sem, out_sem,
    data, relay_box, sums, fin, from_partner, z_in, x_in, direct_in, nyq_box, nyq_rows,
    buf, zbuf, ebuf, psum, mean_out, mean_in,
    load_sem, swap_send, swap_recv, halo_send, halo_recv, relay_send, relay_recv,
    z_send, z_recv, x_send, x_recv, direct_send, direct_recv, core_send, core_recv, mean_send, mean_recv,
):
    chan, chan_count = lax.axis_index("chan"), lax.axis_size("chan")
    me = lax.axis_index("tm")
    core = lax.rem(me, CORES)
    chip = me // CORES
    chips = lax.axis_size("tm") // CORES
    z, x = chip // SPAN, lax.rem(chip, SPAN)
    half_len = ROOT * HALF
    block_len = 2 * half_len
    mine = data.shape[0]
    groups = mine // ROWS
    tile = ROWS // 2
    batches = groups // 2
    ringed = groups
    size = tile * ROWS
    inner = jnp.logical_and(x > 0, x < SPAN - 1)
    has_left, has_right = chip > 0, chip < chips - 1
    exists = (has_right, has_left)

    def as_int(flag):
        return flag.astype(jnp.int32)

    def device(chip_index, core_index):
        return {"tm": chip_index * CORES + core_index}

    def z_peer(step):
        return device(lax.rem(z + step + SPAN, SPAN) * SPAN + x, core)

    def x_peer(step):
        return device(z * SPAN + lax.rem(x + step + SPAN, SPAN), core)

    partner = device(chip, 1 - core)
    toward = 2 * core - 1
    sends_halo = jnp.where(core == 0, as_int(has_left), as_int(has_right)) == 1
    at_column = jnp.logical_or(x == 0, x == SPAN - 1)
    has_next_row = jnp.where(core == 0, as_int(z > 0), as_int(z < SPAN - 1)) == 1
    linked = jnp.logical_and(at_column, has_next_row)
    crosses = jnp.logical_and(linked, x == (SPAN - 1) * core)
    relays = jnp.logical_and(linked, x == (SPAN - 1) * (1 - core))
    faces = x == (SPAN - 1) * (1 - core)
    next_row = device(chip + toward * SPAN, 1 - core)

    def across(core_index):
        return device(z * SPAN + (SPAN - 1) - x, core_index)

    def remote(source, target, send, recv, where):
        return pltpu.make_async_remote_copy(
            src_ref=source, dst_ref=target, send_sem=send, recv_sem=recv,
            device_id=where, device_id_type=pl.DeviceIdType.MESH,
        )

    def strip(g):
        return pl.ds(pl.multiple_of(g * ROWS, ROWS), ROWS)

    def columns(g, side):
        start = side * half_len + core * block_len
        return pl.ds(pl.multiple_of(start, half_len), block_len)

    def load(g):
        rows = pl.ds(pl.multiple_of(core * mine + g * ROWS, ROWS), ROWS)
        place = data.at[strip(g), columns(g, lax.rem(g + core, 2))]
        return pltpu.make_async_copy(strain_ref.at[rows], place, load_sem.at[g])

    def swap(g):
        rows = pl.ds(pl.multiple_of((1 - core) * mine + g * ROWS, ROWS), ROWS)
        place = data.at[strip(g), columns(g, lax.rem(g + 1 - core, 2))]
        return remote(strain_ref.at[rows], place, swap_send, swap_recv.at[g], partner)

    def halo_group(n, side, to):
        return 2 * n + lax.rem(side + to, 2)

    def halo_place(n, side, to):
        start = (1 - side) * 2 * CORES * half_len
        return data.at[strip(halo_group(n, side, to)), pl.ds(pl.multiple_of(start, half_len), half_len)]

    def halo_source(n, to):
        return strain_ref.at[
            pl.ds(pl.multiple_of(to * mine + halo_group(n, core, to) * ROWS, ROWS), ROWS),
            pl.ds(pl.multiple_of(core * half_len, half_len), half_len),
        ]

    def halo_copy(n, to):
        return remote(
            halo_source(n, to), halo_place(n, core, to), halo_send, halo_recv.at[core, n],
            device(chip + toward, to),
        )

    def relay_copy(k, to):
        n = RELAYED[k]
        return remote(
            halo_source(n, to), relay_box.at[k, to], halo_send, relay_recv.at[k, to], next_row
        )

    def relay_on(k, to):
        n = RELAYED[k]
        return remote(
            relay_box.at[k, to], halo_place(n, 1 - core, to), relay_send,
            halo_recv.at[1 - core, n], across(to),
        )

    def halo_arrival(n, side):
        block = halo_place(n, side, core)
        return remote(block, block, halo_send, halo_recv.at[side, n], partner)

    barrier = pltpu.get_barrier_semaphore()

    def greet(where):
        pl.semaphore_signal(barrier, inc=1, device_id=where, device_id_type=pl.DeviceIdType.MESH)

    def mean_peer(other, k):
        where = {"chan": lax.rem(chan + k, chan_count)}
        if other:
            where["tm"] = chip * CORES + 1 - core
        return where

    def chip_peer(k):
        far_z, far_x = lax.rem(z + k // SPAN, SPAN), lax.rem(x + k % SPAN, SPAN)
        return far_z, far_x, device(far_z * SPAN + far_x, core)

    greet(partner)
    for k in range(1, SPAN * SPAN):
        greet(chip_peer(k)[2])
    for k in range(1, chan_count):
        for other in range(2):
            greet(mean_peer(other, k))
    for flag, shift, both in ((has_left, -1, 0), (has_right, 1, 1)):
        @pl.when(flag)
        def _():
            greet(device(chip + shift, 1 - both))

            @pl.when(core == both)
            def _():
                greet(device(chip + shift, both))

    @pl.when(linked)
    def _():
        greet(next_row)

    @pl.when(faces)
    def _():
        greet(across(1 - core))

    tables_in = [
        pltpu.make_async_copy(source, target, table_sem.at[n])
        for n, (source, target) in enumerate(
            zip(
                (window_hbm, first_hbm, second_hbm, twist_hbm, mirror_hbm),
                (window_ref, first_ref, second_ref, twist_ref, mirror_ref),
            )
        )
    ]
    load(0).start()
    for table in tables_in:
        table.start()

    @pl.loop(1, groups)
    def _(g):
        load(g).start()

    left_count = as_int(has_left) * (2 - core)
    right_count = as_int(has_right) * (1 + core)
    pl.semaphore_wait(
        barrier,
        left_count + right_count + as_int(linked) + as_int(faces) + SPAN * SPAN + 2 * (chan_count - 1),
    )

    for n in range(batches):
        for side in range(2):
            swap(2 * n + side).start()

        @pl.when(sends_halo)
        def _():
            for turn in range(CORES):
                to = lax.rem(core + turn, CORES)
                if n in RELAYED:
                    @pl.when(crosses)
                    def _():
                        relay_copy(RELAYED.index(n), to).start()

                    @pl.when(jnp.logical_not(crosses))
                    def _():
                        halo_copy(n, to).start()
                elif n == HELD:
                    @pl.when(jnp.logical_not(crosses))
                    def _():
                        halo_copy(n, to).start()
                else:
                    halo_copy(n, to).start()

    nyq_rows[...] = jnp.zeros_like(nyq_rows)
    for table in tables_in:
        table.wait()
    consts = (window_ref, first_ref, second_ref, twist_ref)
    scratch = (buf, zbuf, ebuf, psum)

    def slab(i, size):
        return pl.ds(pl.multiple_of(i * size, size), size)

    def way(i):
        return 1 - 2 * lax.rem(i, 2)

    def z_block(i, step):
        return sums.at[slab(i, tile), lax.rem(z + step + SPAN, SPAN)]

    def x_block(i, step):
        return sums.at[slab(i, tile), z, lax.rem(x + step + SPAN, SPAN)]

    def ring(kind, i, block, inbox, send, recv, peer):
        d = way(i)
        step, hop = ((2, d), (-d, -d), (d, d))[kind]
        return remote(block(i, step), inbox.at[kind, i], send, recv.at[kind, i], peer(hop))

    def z_copy(kind, i):
        return ring(kind, i, z_block, z_in, z_send, z_recv, z_peer)

    def x_copy(kind, i):
        return ring(kind, i, x_block, x_in, x_send, x_recv, x_peer)

    def core_copy(i):
        count = 2 * size + (ROWS if i == batches - 1 else 0)
        rows = pl.ds(i * 2 * size, count)
        return remote(fin.at[rows], from_partner.at[rows], core_send, core_recv.at[i], partner)

    def direct_copy(k):
        far_z, far_x, where = chip_peer(k)
        return remote(nyq_box, direct_in.at[k], direct_send, direct_recv, where)

    def direct_all():
        box = direct_in.at[pl.ds(1, SPAN * SPAN - 1)]
        return remote(box, box, direct_send, direct_recv, partner)

    def send_direct():
        for k in (10, 6, 9, 11, 14, 2, 8, 5, 7, 13, 15, 1, 3, 4, 12):
            direct_copy(k).start()

    def sum_direct():
        direct_all().wait_recv()
        nyq = jnp.zeros((ROWS, ROOT), jnp.float32)
        for far_z in range(SPAN):
            for far_x in range(SPAN):
                k = lax.rem(z - far_z + SPAN, SPAN) * SPAN + lax.rem(x - far_x + SPAN, SPAN)
                nyq = nyq + direct_in[k]
        fin[pl.ds(groups * size, ROWS), :] = nyq

    def begin(copy, i):
        copy(0, i).start()
        copy(1, i).start()

    def advance(copy, block, inbox, i):
        copy(0, i).wait_recv()
        target = block(i, way(i))
        target[...] = target[...] + inbox[0, i]
        copy(2, i).start()

    def collect(copy, block, inbox, i):
        copy(1, i).wait_recv()
        copy(2, i).wait_recv()
        return block(i, 0)[...] + inbox[1, i] + inbox[2, i]

    def z_advance(i):
        advance(z_copy, z_block, z_in, i)

    def z_collect(i):
        z_block(i, 0)[...] = collect(z_copy, z_block, z_in, i)

    def short_copy(k, i):
        return remote(x_block(i, k), x_in.at[k - 1, i], x_send, x_recv.at[k - 1, i], x_peer(k))

    def short_begin(i):
        for k in (2, 1, 3):
            short_copy(k, i).start()

    def short_collect(i):
        total = x_block(i, 0)[...]
        for k in (1, 3, 2):
            short_copy(k, i).wait_recv()
            total = total + x_in[k - 1, i]
        fin[pl.ds(i * size, size), :] = total.reshape(size, ROOT)

    def x_advance(i):
        advance(x_copy, x_block, x_in, i)

    def x_collect(i):
        rows = pl.ds(pl.multiple_of(i * size, size), size)
        fin[rows, :] = collect(x_copy, x_block, x_in, i).reshape(size, ROOT)

    @pl.loop(0, groups)
    def _(t):
        side = lax.rem(t + core, 2)
        here = jnp.where(side == 0, as_int(has_right), as_int(has_left))
        load(t).wait()
        swap(t).wait_recv()

        for k in range(len(RELAYED)):
            @pl.when(jnp.logical_and(relays, t == RELAY_AT[k]))
            def _():
                for turn in range(CORES):
                    to = lax.rem(1 - core + turn, CORES)
                    relay_copy(k, to).wait_recv()
                    relay_on(k, to).start()

        @pl.when(jnp.logical_and(crosses, t == HELD))
        def _():
            for turn in range(CORES):
                halo_copy(HELD, lax.rem(core + turn, CORES)).start()

        def wait_halo():
            @pl.when(jnp.logical_and(inner, t >= 2))
            def _():
                z_advance(t - 2)

            for at, first, last in LATE:
                @pl.when(jnp.logical_and(jnp.logical_not(inner), t == at))
                def _():
                    @pl.loop(first, last)
                    def _(i):
                        z_advance(i)

            for at, first, last in X_START:
                @pl.when(t == at)
                def _():
                    @pl.loop(first, last)
                    def _(i):
                        z_collect(i)
                        begin(x_copy, i)

            @pl.when(t == groups - 1)
            def _():
                @pl.loop(0, 4)
                def _(i):
                    x_advance(i)

            @pl.when(here == 1)
            def _():
                halo_arrival(t // 2, side).wait_recv()

            @pl.when(here == 0)
            def _():
                place = halo_place(t // 2, side, core)
                place[...] = jnp.zeros((ROWS, half_len), jnp.float32)

        nyq = group_sums(side, data.at[strip(t)], here.astype(jnp.float32), wait_halo, consts, scratch)
        nyq_rows[strip(t), :] = jnp.broadcast_to(nyq, (ROWS, ROOT))
        for p in range(tile):
            turned = jnp.transpose(psum[p * ROOT : (p + 1) * ROOT, :])
            sums[t * tile + p] = turned.reshape(sums.shape[1:])

        begin(z_copy, t)

    nyq_box[...] = jnp.transpose(nyq_rows[...])[:ROWS]
    direct_in[0] = nyq_box[...]
    z_advance(10)
    send_direct()
    x_advance(4)
    x_advance(5)
    z_collect(8)
    short_begin(8)
    for i in range(4):
        x_collect(i)
    core_copy(0).start()
    core_copy(1).start()
    x_advance(6)
    x_advance(7)
    z_collect(9)
    short_begin(9)
    z_advance(11)
    x_collect(4)
    x_collect(5)
    core_copy(2).start()
    z_collect(10)
    short_begin(10)
    x_collect(6)
    x_collect(7)
    core_copy(3).start()
    short_collect(8)
    short_collect(9)
    core_copy(4).start()

    lanes = lax.broadcasted_iota(jnp.int32, (1, ROOT), 1)
    factors = [jnp.where(jnp.logical_and(lanes == 0, me + j == 0), scale, 2.0 * scale) for j in range(2)]

    def unfold(both):
        high = both.astype(jnp.bfloat16)
        middle = (both - high.astype(jnp.float32)).astype(jnp.bfloat16)
        low = (both - high.astype(jnp.float32) - middle.astype(jnp.float32)).astype(jnp.bfloat16)
        parts = [jnp.dot(part, mirror_ref[...], preferred_element_type=jnp.float32) for part in (low, middle, high)]
        return parts[0] + parts[1] + parts[2]

    def spread(block, owner, first, count):
        for j in range(2):
            both = jnp.concatenate(
                [block[pl.ds(SPAN * core + j + shift + first * ROWS, count, stride=ROWS), :] for shift in (0, 2)],
                axis=1,
            )
            placed = unfold(both)
            for half in range(2):
                at = j * CORES * mine + owner * mine + 2 * first + half
                power_box[pl.ds(at, count, stride=2), :] = placed[:, half * ROOT : (half + 1) * ROOT] * factors[j]

    def add_tiles(first, last):
        lines = [fin[slab(i, ROWS), :] for i in range(first, last)]
        while len(lines) > 1:
            lines = [a + b for a, b in zip(lines[::2], lines[1::2])] + lines[len(lines) // 2 * 2 :]
        return lines[0]

    most = 10 * tile
    spread(fin, core, 0, most)
    early = add_tiles(0, most)
    z_collect(11)
    short_begin(11)
    short_collect(10)
    for b in range(batches - 1):
        core_copy(b).wait_recv()
    spread(from_partner, 1 - core, 0, most)
    sum_direct()
    short_collect(11)
    core_copy(5).start()
    mean_out[...] = early + add_tiles(most, groups * tile)

    def mean_copy(other, k):
        return remote(
            mean_out, mean_in.at[other, k], mean_send.at[other, k], mean_recv.at[other, k], mean_peer(other, k)
        )

    mean_links = [(other, k) for other in range(2) for k in range(chan_count) if other + k > 0]
    for link in mean_links:
        mean_copy(*link).start()
    mean_in[0, 0] = mean_out[...]
    spread(fin, core, most, groups * tile - most)
    core_copy(batches - 1).wait_recv()
    spread(from_partner, 1 - core, most, groups * tile - most)
    power_out = pltpu.make_async_copy(power_box, packed_ref.at[: power_box.shape[0]], out_sem.at[0])
    power_out.start()

    ends = [
        ref[groups * size : groups * size + 1, :] * scale for ref in (fin, from_partner)
    ]
    parts = [jnp.where(core == source, ends[0], ends[1]) for source in range(CORES)]
    moved = pltpu.roll(parts[1], mine, 1)
    small_box[...] = jnp.zeros_like(small_box)
    small_box[0:1, :] = jnp.where(lanes < mine, parts[0], moved)
    small_box[1:2, :] = moved

    def sent(box, send):
        remote(box, box, send, core_recv.at[0], partner).wait_send()

    sent(strain_ref.at[pl.ds(0, mine)], swap_send)
    sent(z_in, z_send)
    sent(x_in, x_send)
    sent(fin, core_send)
    direct_all().wait_send()

    @pl.when(sends_halo)
    def _():
        sent(strain_ref.at[pl.ds(0, mine), pl.ds(0, half_len)], halo_send)

    @pl.when(relays)
    def _():
        sent(relay_box, relay_send)

    for link in mean_links:
        mean_copy(*link).wait()
    total = jnp.zeros((ROWS, ROOT), jnp.float32)
    for source_chan in range(chan_count):
        for source_core in range(CORES):
            total = total + mean_in[
                lax.rem(core + source_core, CORES), lax.rem(chan - source_chan + chan_count, chan_count)
            ]
    mean_out[...] = total
    rows = [mean_out[pl.ds(SPAN * core + j, 1), :] for j in range(SPAN)]
    placed = unfold(
        jnp.concatenate(
            [jnp.concatenate([rows[j], rows[j + 2]], axis=1) for j in range(2)]
            + [jnp.zeros((ROWS - 2, 2 * ROOT), jnp.float32)],
            axis=0,
        )
    )
    placed = placed[:, :ROOT] + placed[:, ROOT:]
    for j in range(2):
        small_box[2 + j : 3 + j, :] = placed[j : j + 1] * (factors[j] * (1.0 / (CORES * mine * chan_count)))
    small_out = pltpu.make_async_copy(small_box, packed_ref.at[power_box.shape[0] :], out_sem.at[1])
    small_out.start()
    power_out.wait()
    small_out.wait()


def finish_kernel(packed_ref, power_ref, nyquist_ref, mean_ref):
    chan_rows = power_ref.shape[0]
    for j in range(2):
        power_ref[:, j * ROOT : (j + 1) * ROOT] = packed_ref[j * chan_rows : (j + 1) * chan_rows, :]
        mean_ref[:, j * ROOT : (j + 1) * ROOT] = packed_ref[2 * chan_rows + 2 + j : 2 * chan_rows + 3 + j, :]
    nyquist_ref[:, :ROOT] = packed_ref[2 * chan_rows : 2 * chan_rows + 1, :]
    nyquist_ref[:, ROOT:] = packed_ref[2 * chan_rows + 1 : 2 * chan_rows + 2, : chan_rows - ROOT]


def per_device(strain):
    chan_rows, time_width = strain.shape
    seg_len = ROOT * ROOT
    half_len = seg_len // 2
    tm_count = lax.axis_size("tm")
    mine = chan_rows // CORES
    assert time_width == seg_len and tm_count == SPAN * SPAN * CORES and mine == 12 * ROWS
    segments = 2 * tm_count - 1
    first_all, second_all, twist, window, mirror, energy = tables(tm_count)
    pairs = mine // 2
    groups = mine // ROWS
    batches = groups // 2
    tile = ROWS // 2
    chan_count = lax.axis_size("chan")
    vmem = pl.BlockSpec(memory_space=pltpu.VMEM)
    f32 = jnp.float32
    dma = pltpu.SemaphoreType.DMA
    relayed = len(RELAYED)
    tables_in = (window, first_all, second_all, twist, mirror)
    packed = pl.pallas_call(
        functools.partial(welch_kernel, 1.0 / (segments * energy)),
        in_specs=[pl.BlockSpec(memory_space=pl.ANY)] * 6,
        out_specs=pl.BlockSpec(memory_space=pl.ANY),
        out_shape=jax.ShapeDtypeStruct((2 * chan_rows + ROWS, ROOT), f32),
        scratch_shapes=[pltpu.VMEM(table.shape, table.dtype) for table in tables_in]
        + [
            pltpu.VMEM((2 * chan_rows, ROOT), f32),
            pltpu.VMEM((ROWS, ROOT), f32),
            dma((len(tables_in),)),
            dma((2,)),
            pltpu.VMEM((mine, CORES * seg_len + half_len), f32),
            pltpu.VMEM((relayed, CORES, ROWS, half_len), f32),
            pltpu.VMEM((pairs, SPAN, SPAN, ROWS, ROOT), f32),
            pltpu.VMEM(((pairs + 1) * ROWS, ROOT), f32),
            pltpu.VMEM(((pairs + 1) * ROWS, ROOT), f32),
            pltpu.VMEM((3, groups, tile, SPAN, ROWS, ROOT), f32),
            pltpu.VMEM((3, groups, tile, ROWS, ROOT), f32),
            pltpu.VMEM((SPAN * SPAN, ROWS, ROOT), f32),
            pltpu.VMEM((ROWS, ROOT), f32),
            pltpu.VMEM((ROOT, ROOT), f32),
            pltpu.VMEM((ROWS * ROOT, ROOT), f32),
            pltpu.VMEM((ROWS * 2 * CORES * HALF, 4 * ROOT), jnp.bfloat16),
            pltpu.VMEM((2 * CORES * ROWS, 6 * ROOT), jnp.bfloat16),
            pltpu.VMEM((ROWS * HALF, ROOT), f32),
            pltpu.VMEM((ROWS, ROOT), f32),
            pltpu.VMEM((2, chan_count, ROWS, ROOT), f32),
            dma((groups,)),
            dma(()),
            dma((groups,)),
            dma(()),
            dma((2, batches)),
            dma(()),
            dma((relayed, CORES)),
            dma(()),
            dma((3, groups)),
            dma(()),
            dma((3, groups)),
            dma(()),
            dma(()),
            dma(()),
            dma((batches,)),
            dma((2, chan_count)),
            dma((2, chan_count)),
        ],
        compiler_params=pltpu.CompilerParams(
            collective_id=0, has_side_effects=True, vmem_limit_bytes=60 * 2**20
        ),
        name="welch",
    )(strain, *tables_in)
    power, nyquist, mean_power = pl.pallas_call(
        finish_kernel,
        in_specs=[vmem],
        out_specs=[vmem] * 3,
        out_shape=[
            jax.ShapeDtypeStruct((chan_rows, 2 * ROOT), f32),
            jax.ShapeDtypeStruct((1, chan_rows), f32),
            jax.ShapeDtypeStruct((1, 2 * ROOT), f32),
        ],
        name="finish",
    )(packed)
    return (power, nyquist.reshape(-1), mean_power.reshape(-1))


def solution(mesh):
    in_specs = (P("chan", "tm"),)
    out_specs = (P("chan", "tm"), P("chan"), P("tm"))
    return jax.shard_map(
        per_device, mesh=mesh, in_specs=in_specs, out_specs=out_specs, check_vma=False
    )
```

```python
import functools

import jax
import jax.numpy as jnp
import numpy as np
from jax import lax
from jax.experimental import pallas as pl
from jax.experimental.pallas import tpu as pltpu
from jax.sharding import PartitionSpec as P

ROOT = 128
HALF = ROOT // 2
ROWS = 8


def split_np(table):
    table = table.astype(np.float32)
    high = table.astype(jnp.bfloat16)
    low = (table - high.astype(np.float32)).astype(jnp.bfloat16)
    return high, low


@functools.cache
def tables(tm_count):
    pos = np.arange(ROOT)
    short = 2.0 * np.pi * (np.outer(pos, pos) % ROOT) / ROOT
    cos_s, sin_s = np.cos(short), np.sin(short)
    first = np.concatenate([cos_s[:HALF], -sin_s[:HALF]], axis=0)
    first_hi, first_lo = split_np(first)
    first_all = np.concatenate(
        [
            np.concatenate([first_hi, first_hi], axis=1),
            np.concatenate([first_lo, first_lo], axis=1),
        ],
        axis=0,
    )
    bands = np.arange(HALF).reshape(tm_count, HALF // tm_count)
    order = np.concatenate([bands, ROOT - 1 - bands], axis=1).reshape(-1)
    cos_o, sin_o = cos_s[:, order], sin_s[:, order]
    second = np.concatenate(
        [np.concatenate([cos_o, -sin_o], axis=1), np.concatenate([sin_o, cos_o], axis=1)], axis=0
    )
    second_hi, second_lo = split_np(second)
    second_all = np.concatenate([second_hi, second_hi, second_lo], axis=0)
    long = 2.0 * np.pi * np.outer(np.arange(HALF + ROWS), pos) / (ROOT * ROOT)
    twist = np.concatenate([np.cos(long), np.sin(long)], axis=1).astype(np.float32)
    mirror = np.zeros((2 * ROOT, 2 * ROOT), np.float32)
    for side in range(2):
        for k in range(HALF):
            mirror[side * HALF + k, side * ROOT + k] = 1.0
            mirror[ROOT + side * HALF + k, side * ROOT + (ROOT - k if k else HALF)] = 1.0
    seg_len = ROOT * ROOT
    window = 0.5 - 0.5 * np.cos(2.0 * np.pi * np.arange(seg_len) / seg_len)
    energy = float(np.sum(window * window))
    return first_all, second_all, twist, window.reshape(ROOT, ROOT).astype(np.float32), mirror.astype(jnp.bfloat16), energy


def split(value):
    high = value.astype(jnp.bfloat16)
    low = (value - high.astype(jnp.float32)).astype(jnp.bfloat16)
    return high, low


SPAN = 4
CORES = 2


RELAYED = (2, 4, 5)
RELAY_AT = (2, 5, 7)
HELD = 3
LATE = ((7, 0, 4), (8, 4, 6), (9, 6, 7), (10, 7, 9), (11, 9, 10))
SHORT = 8
X_START = ((9, 0, 4), (10, 4, 6), (11, 6, 8))


def half_sum(ref):
    parts = [ref[:, ROOT * a : ROOT * (a + 1)] for a in range(HALF)]
    while len(parts) > 1:
        parts = [parts[n] + parts[n + 1] for n in range(0, len(parts), 2)]
    return jnp.sum(parts[0], axis=1, keepdims=True)


def stage_one(piece, mean, consts, buf, zbuf, ebuf, seg, segs):
    window_ref, first_ref, _, twist_ref = consts
    mean = jnp.broadcast_to(mean, (ROWS, ROOT))
    even = jnp.zeros((ROWS, ROOT), jnp.float32)
    odd = jnp.zeros((ROWS, ROOT), jnp.float32)
    for a in range(ROOT):
        tile = (piece[:, ROOT * a : ROOT * (a + 1)] - mean) * window_ref[a : a + 1, :]
        buf[ROWS * a : ROWS * (a + 1), :] = tile
        if a % 2 == 0:
            even = even + tile
        else:
            odd = odd + tile
    alt = even - odd
    sign = (1 - 2 * (lax.broadcasted_iota(jnp.int32, (ROWS, ROOT), 1) % 2)).astype(jnp.float32)
    edge = jnp.sum((even + odd) * sign, axis=1, keepdims=True)
    turn = twist_ref[HALF : HALF + 1, :]
    high, low = split(jnp.concatenate([alt * turn[:, :ROOT], -alt * turn[:, ROOT:]], axis=1))
    ebuf[seg * ROWS : (seg + 1) * ROWS, :] = jnp.concatenate([high, low, high], axis=1)
    cos_t, sin_t = twist_ref[:HALF, :ROOT], twist_ref[:HALF, ROOT:]
    for r in range(0, ROWS, 2):
        pair = jnp.concatenate(
            [buf[pl.ds(r, ROOT, stride=ROWS), :], buf[pl.ds(r + 1, ROOT, stride=ROWS), :]], axis=1
        )
        high, low = split(pair)
        out = jnp.dot(
            first_ref[...], jnp.concatenate([high, low], axis=0), preferred_element_type=jnp.float32
        )
        out = out[:ROOT] + out[ROOT:]
        for s in range(2):
            re = out[:HALF, s * ROOT : (s + 1) * ROOT]
            im = out[HALF:, s * ROOT : (s + 1) * ROOT]
            z_hi, z_lo = split(
                jnp.concatenate([re * cos_t + im * sin_t, im * cos_t - re * sin_t], axis=1)
            )
            at = ((r + s) * segs + seg) * HALF
            zbuf[at : at + HALF, 0 : 2 * ROOT] = z_hi
            zbuf[at : at + HALF, 2 * ROOT :] = z_lo
    return edge * edge


def squares(left, right):
    out = jnp.dot(left, right, preferred_element_type=jnp.float32)
    return out[:, :ROOT] * out[:, :ROOT] + out[:, ROOT:] * out[:, ROOT:]


def group_sums(side, rows, on, wait_halo, consts, scratch):
    second_ref = consts[2]
    buf, zbuf, ebuf, psum = scratch
    half_len = ROOT * HALF
    segs = 2 * CORES
    lane = lax.broadcasted_iota(jnp.int32, (ROWS, ROOT), 1)

    def window(start, length):
        return rows.at[:, pl.ds(pl.multiple_of(start, half_len), length)]

    own = side * half_len
    totals = [half_sum(window(own + h * half_len, half_len)) for h in range(segs)]
    inverse = 1.0 / (2 * half_len)
    nyq = jnp.zeros((ROWS, 1), jnp.float32)
    for seg in range(segs - 1):
        nyq = nyq + stage_one(
            window(own + seg * half_len, 2 * half_len), (totals[seg] + totals[seg + 1]) * inverse,
            consts, buf, zbuf, ebuf, seg, segs,
        )
    wait_halo()
    near = jnp.where(side == 0, totals[-1], totals[0])
    far = half_sum(window((1 - side) * segs * half_len, half_len))
    nyq = nyq + on * stage_one(
        window((1 - side) * (segs - 1) * half_len, 2 * half_len), (near + far) * inverse,
        consts, buf, zbuf, ebuf, segs - 1, segs,
    )

    def fold(power, count):
        total = power[:count]
        for seg in range(1, segs - 1):
            total = total + power[seg * count : (seg + 1) * count]
        return total + on * power[(segs - 1) * count :]

    for r in range(ROWS):
        at = slice(r * segs * HALF, (r + 1) * segs * HALF)
        left = jnp.concatenate([zbuf[at, :], zbuf[at, : 2 * ROOT]], axis=1)
        psum[r * HALF : (r + 1) * HALF, :] = fold(squares(left, second_ref[...]), HALF)
    mixed = fold(squares(ebuf[...], second_ref[...]), ROWS)
    first_rows = pl.ds(0, ROWS, stride=HALF)
    psum[first_rows, :] = jnp.where(lane % SPAN >= SPAN // 2, mixed, psum[first_rows, :])
    return nyq


def welch_kernel(
    scale, strain_ref, window_hbm, first_hbm, second_hbm, twist_hbm, mirror_hbm, packed_ref,
    window_ref, first_ref, second_ref, twist_ref, mirror_ref, power_box, small_box, table_sem, out_sem,
    data, relay_box, sums, fin, from_partner, z_in, x_in, direct_in, direct_out, group_sum, group_in, nyq_rows,
    buf, zbuf, ebuf, psum,
    load_sem, swap_send, swap_recv, halo_send, halo_recv, relay_send, relay_recv,
    z_send, z_recv, x_send, x_recv, direct_send, direct_recv, core_send, core_recv, mean_send, mean_recv,
):
    chan, chan_count = lax.axis_index("chan"), lax.axis_size("chan")
    me = lax.axis_index("tm")
    core = lax.rem(me, CORES)
    chip = me // CORES
    chips = lax.axis_size("tm") // CORES
    z, x = chip // SPAN, lax.rem(chip, SPAN)
    half_len = ROOT * HALF
    block_len = 2 * half_len
    mine = data.shape[0]
    groups = mine // ROWS
    tile = ROWS // 2
    batches = groups // 2
    ringed = groups
    size = tile * ROWS
    inner = jnp.logical_and(x > 0, x < SPAN - 1)
    has_left, has_right = chip > 0, chip < chips - 1
    exists = (has_right, has_left)

    def as_int(flag):
        return flag.astype(jnp.int32)

    def device(chip_index, core_index):
        return {"tm": chip_index * CORES + core_index}

    def z_peer(step):
        return device(lax.rem(z + step + SPAN, SPAN) * SPAN + x, core)

    def x_peer(step):
        return device(z * SPAN + lax.rem(x + step + SPAN, SPAN), core)

    partner = device(chip, 1 - core)
    toward = 2 * core - 1
    sends_halo = jnp.where(core == 0, as_int(has_left), as_int(has_right)) == 1
    at_column = jnp.logical_or(x == 0, x == SPAN - 1)
    has_next_row = jnp.where(core == 0, as_int(z > 0), as_int(z < SPAN - 1)) == 1
    linked = jnp.logical_and(at_column, has_next_row)
    crosses = jnp.logical_and(linked, x == (SPAN - 1) * core)
    relays = jnp.logical_and(linked, x == (SPAN - 1) * (1 - core))
    faces = x == (SPAN - 1) * (1 - core)
    next_row = device(chip + toward * SPAN, 1 - core)

    def across(core_index):
        return device(z * SPAN + (SPAN - 1) - x, core_index)

    def remote(source, target, send, recv, where):
        return pltpu.make_async_remote_copy(
            src_ref=source, dst_ref=target, send_sem=send, recv_sem=recv,
            device_id=where, device_id_type=pl.DeviceIdType.MESH,
        )

    def strip(g):
        return pl.ds(pl.multiple_of(g * ROWS, ROWS), ROWS)

    def columns(g, side):
        start = side * half_len + core * block_len
        return pl.ds(pl.multiple_of(start, half_len), block_len)

    def load(g):
        rows = pl.ds(pl.multiple_of(core * mine + g * ROWS, ROWS), ROWS)
        place = data.at[strip(g), columns(g, lax.rem(g + core, 2))]
        return pltpu.make_async_copy(strain_ref.at[rows], place, load_sem.at[g])

    def swap(g):
        rows = pl.ds(pl.multiple_of((1 - core) * mine + g * ROWS, ROWS), ROWS)
        place = data.at[strip(g), columns(g, lax.rem(g + 1 - core, 2))]
        return remote(strain_ref.at[rows], place, swap_send, swap_recv.at[g], partner)

    def halo_group(n, side, to):
        return 2 * n + lax.rem(side + to, 2)

    def halo_place(n, side, to):
        start = (1 - side) * 2 * CORES * half_len
        return data.at[strip(halo_group(n, side, to)), pl.ds(pl.multiple_of(start, half_len), half_len)]

    def halo_source(n, to):
        return strain_ref.at[
            pl.ds(pl.multiple_of(to * mine + halo_group(n, core, to) * ROWS, ROWS), ROWS),
            pl.ds(pl.multiple_of(core * half_len, half_len), half_len),
        ]

    def halo_copy(n, to):
        return remote(
            halo_source(n, to), halo_place(n, core, to), halo_send, halo_recv.at[core, n],
            device(chip + toward, to),
        )

    def relay_copy(k, to):
        n = RELAYED[k]
        return remote(
            halo_source(n, to), relay_box.at[k, to], halo_send, relay_recv.at[k, to], next_row
        )

    def relay_on(k, to):
        n = RELAYED[k]
        return remote(
            relay_box.at[k, to], halo_place(n, 1 - core, to), relay_send,
            halo_recv.at[1 - core, n], across(to),
        )

    def halo_arrival(n, side):
        block = halo_place(n, side, core)
        return remote(block, block, halo_send, halo_recv.at[side, n], partner)

    barrier = pltpu.get_barrier_semaphore()

    def greet(where):
        pl.semaphore_signal(barrier, inc=1, device_id=where, device_id_type=pl.DeviceIdType.MESH)

    def chan_peer(k):
        return {"chan": lax.rem(chan + k, chan_count)}

    def chip_peer(k):
        far_z, far_x = lax.rem(z + k // SPAN, SPAN), lax.rem(x + k % SPAN, SPAN)
        return far_z, far_x, device(far_z * SPAN + far_x, core)

    greet(partner)
    for k in range(1, SPAN * SPAN):
        greet(chip_peer(k)[2])
    for k in range(1, chan_count):
        greet(chan_peer(k))
    for flag, shift, both in ((has_left, -1, 0), (has_right, 1, 1)):
        @pl.when(flag)
        def _():
            greet(device(chip + shift, 1 - both))

            @pl.when(core == both)
            def _():
                greet(device(chip + shift, both))

    @pl.when(linked)
    def _():
        greet(next_row)

    @pl.when(faces)
    def _():
        greet(across(1 - core))

    tables_in = [
        pltpu.make_async_copy(source, target, table_sem.at[n])
        for n, (source, target) in enumerate(
            zip(
                (window_hbm, first_hbm, second_hbm, twist_hbm, mirror_hbm),
                (window_ref, first_ref, second_ref, twist_ref, mirror_ref),
            )
        )
    ]
    load(0).start()
    for table in tables_in:
        table.start()

    @pl.loop(1, groups)
    def _(g):
        load(g).start()

    left_count = as_int(has_left) * (2 - core)
    right_count = as_int(has_right) * (1 + core)
    pl.semaphore_wait(
        barrier,
        left_count + right_count + as_int(linked) + as_int(faces) + SPAN * SPAN + chan_count - 1,
    )

    for n in range(batches):
        for side in range(2):
            swap(2 * n + side).start()

        @pl.when(sends_halo)
        def _():
            for turn in range(CORES):
                to = lax.rem(core + turn, CORES)
                if n in RELAYED:
                    @pl.when(crosses)
                    def _():
                        relay_copy(RELAYED.index(n), to).start()

                    @pl.when(jnp.logical_not(crosses))
                    def _():
                        halo_copy(n, to).start()
                elif n == HELD:
                    @pl.when(jnp.logical_not(crosses))
                    def _():
                        halo_copy(n, to).start()
                else:
                    halo_copy(n, to).start()

    nyq_rows[...] = jnp.zeros_like(nyq_rows)
    group_sum[...] = jnp.zeros_like(group_sum)
    for table in tables_in:
        table.wait()
    consts = (window_ref, first_ref, second_ref, twist_ref)
    scratch = (buf, zbuf, ebuf, psum)

    def slab(i, size):
        return pl.ds(pl.multiple_of(i * size, size), size)

    def way(i):
        return 1 - 2 * lax.rem(i, 2)

    def z_block(i, step):
        return sums.at[slab(i, tile), lax.rem(z + step + SPAN, SPAN)]

    def x_block(i, step):
        return sums.at[slab(i, tile), z, lax.rem(x + step + SPAN, SPAN)]

    def ring(kind, i, block, inbox, send, recv, peer):
        d = way(i)
        step, hop = ((2, d), (-d, -d), (d, d))[kind]
        return remote(block(i, step), inbox.at[kind, i], send, recv.at[kind, i], peer(hop))

    def z_copy(kind, i):
        return ring(kind, i, z_block, z_in, z_send, z_recv, z_peer)

    def x_copy(kind, i):
        return ring(kind, i, x_block, x_in, x_send, x_recv, x_peer)

    def core_copy(i):
        count = 2 * size + (2 * ROWS if i == batches - 1 else 0)
        rows = pl.ds(i * 2 * size, count)
        return remote(fin.at[rows], from_partner.at[rows], core_send, core_recv.at[i], partner)

    def direct_copy(k):
        far_z, far_x, where = chip_peer(k)
        return remote(direct_out.at[far_z, far_x], direct_in.at[k], direct_send, direct_recv, where)

    def direct_all():
        box = direct_in.at[pl.ds(1, SPAN * SPAN - 1)]
        return remote(box, box, direct_send, direct_recv, partner)

    def send_direct():
        for k in (10, 6, 9, 11, 14, 2, 8, 5, 7, 13, 15, 1, 3, 4, 12):
            direct_copy(k).start()

    def sum_direct():
        direct_all().wait_recv()
        total = jnp.zeros((2, ROWS, ROOT), jnp.float32)
        for far_z in range(SPAN):
            for far_x in range(SPAN):
                k = lax.rem(z - far_z + SPAN, SPAN) * SPAN + lax.rem(x - far_x + SPAN, SPAN)
                total = total + direct_in[k]
        fin[pl.ds(groups * size, 2 * ROWS), :] = total.reshape(2 * ROWS, ROOT)

    def chan_copy(k):
        return remote(group_sum, group_in.at[k], mean_send.at[k], mean_recv.at[k], chan_peer(k))

    def chan_begin():
        for k in (2, 1, 3):
            chan_copy(k).start()
        group_in[0] = group_sum[...]

    def chan_collect():
        for k in range(1, chan_count):
            chan_copy(k).wait_recv()
        total = group_in[lax.rem(chan + chan_count, chan_count)]
        for source in range(1, chan_count):
            total = total + group_in[lax.rem(chan - source + chan_count, chan_count)]
        direct_out[:, :, 1] = total
        direct_in[0] = direct_out[z, x]

    def begin(copy, i):
        copy(0, i).start()
        copy(1, i).start()

    def advance(copy, block, inbox, i):
        copy(0, i).wait_recv()
        target = block(i, way(i))
        target[...] = target[...] + inbox[0, i]
        copy(2, i).start()

    def collect(copy, block, inbox, i):
        copy(1, i).wait_recv()
        copy(2, i).wait_recv()
        return block(i, 0)[...] + inbox[1, i] + inbox[2, i]

    def z_advance(i):
        advance(z_copy, z_block, z_in, i)

    def z_collect(i):
        z_block(i, 0)[...] = collect(z_copy, z_block, z_in, i)

    def short_copy(k, i):
        return remote(x_block(i, k), x_in.at[k - 1, i], x_send, x_recv.at[k - 1, i], x_peer(k))

    def short_begin(i):
        for k in (2, 1, 3):
            short_copy(k, i).start()

    def short_collect(i):
        total = x_block(i, 0)[...]
        for k in (1, 3, 2):
            short_copy(k, i).wait_recv()
            total = total + x_in[k - 1, i]
        fin[pl.ds(i * size, size), :] = total.reshape(size, ROOT)

    def x_advance(i):
        advance(x_copy, x_block, x_in, i)

    def x_collect(i):
        rows = pl.ds(pl.multiple_of(i * size, size), size)
        fin[rows, :] = collect(x_copy, x_block, x_in, i).reshape(size, ROOT)

    @pl.loop(0, groups)
    def _(t):
        side = lax.rem(t + core, 2)
        here = jnp.where(side == 0, as_int(has_right), as_int(has_left))
        load(t).wait()
        swap(t).wait_recv()

        for k in range(len(RELAYED)):
            @pl.when(jnp.logical_and(relays, t == RELAY_AT[k]))
            def _():
                for turn in range(CORES):
                    to = lax.rem(1 - core + turn, CORES)
                    relay_copy(k, to).wait_recv()
                    relay_on(k, to).start()

        @pl.when(jnp.logical_and(crosses, t == HELD))
        def _():
            for turn in range(CORES):
                halo_copy(HELD, lax.rem(core + turn, CORES)).start()

        def wait_halo():
            @pl.when(jnp.logical_and(inner, t >= 2))
            def _():
                z_advance(t - 2)

            for at, first, last in LATE:
                @pl.when(jnp.logical_and(jnp.logical_not(inner), t == at))
                def _():
                    @pl.loop(first, last)
                    def _(i):
                        z_advance(i)

            for at, first, last in X_START:
                @pl.when(t == at)
                def _():
                    @pl.loop(first, last)
                    def _(i):
                        z_collect(i)
                        begin(x_copy, i)

            @pl.when(t == groups - 1)
            def _():
                @pl.loop(0, 4)
                def _(i):
                    x_advance(i)

            @pl.when(here == 1)
            def _():
                halo_arrival(t // 2, side).wait_recv()

            @pl.when(here == 0)
            def _():
                place = halo_place(t // 2, side, core)
                place[...] = jnp.zeros((ROWS, half_len), jnp.float32)

        nyq = group_sums(side, data.at[strip(t)], here.astype(jnp.float32), wait_halo, consts, scratch)
        nyq_rows[strip(t), :] = jnp.broadcast_to(nyq, (ROWS, ROOT))
        added = group_sum[...]
        for p in range(tile):
            turned = jnp.transpose(psum[p * ROOT : (p + 1) * ROOT, :]).reshape(sums.shape[1:])
            sums[t * tile + p] = turned
            added = added + turned
        group_sum[...] = added

        begin(z_copy, t)

    chan_begin()
    direct_out[:, :, 0] = jnp.broadcast_to(
        jnp.transpose(nyq_rows[...])[:ROWS].reshape(1, 1, ROWS, ROOT), (SPAN, SPAN, ROWS, ROOT)
    )
    z_advance(10)
    x_advance(4)
    x_advance(5)
    z_collect(8)
    short_begin(8)
    z_collect(9)
    short_begin(9)
    x_advance(6)
    x_advance(7)
    z_advance(11)
    z_collect(10)
    short_begin(10)
    chan_collect()
    send_direct()
    for i in range(4):
        x_collect(i)
    core_copy(0).start()
    core_copy(1).start()
    z_collect(11)
    short_begin(11)
    x_collect(4)
    x_collect(5)
    core_copy(2).start()
    x_collect(6)
    x_collect(7)
    core_copy(3).start()
    short_collect(8)
    short_collect(9)
    core_copy(4).start()

    lanes = lax.broadcasted_iota(jnp.int32, (1, ROOT), 1)
    factors = [jnp.where(jnp.logical_and(lanes == 0, me + j == 0), scale, 2.0 * scale) for j in range(2)]

    def unfold(both):
        high = both.astype(jnp.bfloat16)
        middle = (both - high.astype(jnp.float32)).astype(jnp.bfloat16)
        low = (both - high.astype(jnp.float32) - middle.astype(jnp.float32)).astype(jnp.bfloat16)
        parts = [jnp.dot(part, mirror_ref[...], preferred_element_type=jnp.float32) for part in (low, middle, high)]
        return parts[0] + parts[1] + parts[2]

    def spread(block, owner, first, count):
        for j in range(2):
            both = jnp.concatenate(
                [block[pl.ds(SPAN * core + j + shift + first * ROWS, count, stride=ROWS), :] for shift in (0, 2)],
                axis=1,
            )
            placed = unfold(both)
            for half in range(2):
                at = j * CORES * mine + owner * mine + 2 * first + half
                power_box[pl.ds(at, count, stride=2), :] = placed[:, half * ROOT : (half + 1) * ROOT] * factors[j]

    most = 10 * tile
    spread(fin, core, 0, most)
    short_collect(10)
    for b in range(batches - 1):
        core_copy(b).wait_recv()
    spread(from_partner, 1 - core, 0, most)
    sum_direct()
    short_collect(11)
    core_copy(5).start()
    spread(fin, core, most, groups * tile - most)
    core_copy(batches - 1).wait_recv()
    spread(from_partner, 1 - core, most, groups * tile - most)
    power_out = pltpu.make_async_copy(power_box, packed_ref.at[: power_box.shape[0]], out_sem.at[0])
    power_out.start()

    ends = [ref[groups * size : groups * size + 1, :] * scale for ref in (fin, from_partner)]
    parts = [jnp.where(core == source, ends[0], ends[1]) for source in range(CORES)]
    moved = pltpu.roll(parts[1], mine, 1)
    small_box[...] = jnp.zeros_like(small_box)
    small_box[0:1, :] = jnp.where(lanes < mine, parts[0], moved)
    small_box[1:2, :] = moved
    rows = []
    for j in range(SPAN):
        at = pl.ds(groups * size + ROWS + SPAN * core + j, 1)
        here, there = fin[at, :], from_partner[at, :]
        rows.append(jnp.where(core == 0, here, there) + jnp.where(core == 0, there, here))
    placed = unfold(
        jnp.concatenate(
            [jnp.concatenate([rows[j], rows[j + 2]], axis=1) for j in range(2)]
            + [jnp.zeros((ROWS - 2, 2 * ROOT), jnp.float32)],
            axis=0,
        )
    )
    placed = placed[:, :ROOT] + placed[:, ROOT:]
    for j in range(2):
        small_box[2 + j : 3 + j, :] = placed[j : j + 1] * (factors[j] * (1.0 / (CORES * mine * chan_count)))
    small_out = pltpu.make_async_copy(small_box, packed_ref.at[power_box.shape[0] :], out_sem.at[1])
    small_out.start()

    def sent(box, send):
        remote(box, box, send, core_recv.at[0], partner).wait_send()

    sent(strain_ref.at[pl.ds(0, mine)], swap_send)
    sent(z_in, z_send)
    sent(x_in, x_send)
    sent(fin, core_send)
    direct_all().wait_send()

    @pl.when(sends_halo)
    def _():
        sent(strain_ref.at[pl.ds(0, mine), pl.ds(0, half_len)], halo_send)

    @pl.when(relays)
    def _():
        sent(relay_box, relay_send)

    for k in range(1, chan_count):
        chan_copy(k).wait_send()
    power_out.wait()
    small_out.wait()


def finish_kernel(packed_ref, power_ref, nyquist_ref, mean_ref):
    chan_rows = power_ref.shape[0]
    for j in range(2):
        power_ref[:, j * ROOT : (j + 1) * ROOT] = packed_ref[j * chan_rows : (j + 1) * chan_rows, :]
        mean_ref[:, j * ROOT : (j + 1) * ROOT] = packed_ref[2 * chan_rows + 2 + j : 2 * chan_rows + 3 + j, :]
    nyquist_ref[:, :ROOT] = packed_ref[2 * chan_rows : 2 * chan_rows + 1, :]
    nyquist_ref[:, ROOT:] = packed_ref[2 * chan_rows + 1 : 2 * chan_rows + 2, : chan_rows - ROOT]


def per_device(strain):
    chan_rows, time_width = strain.shape
    seg_len = ROOT * ROOT
    half_len = seg_len // 2
    tm_count = lax.axis_size("tm")
    mine = chan_rows // CORES
    assert time_width == seg_len and tm_count == SPAN * SPAN * CORES and mine == 12 * ROWS
    segments = 2 * tm_count - 1
    first_all, second_all, twist, window, mirror, energy = tables(tm_count)
    pairs = mine // 2
    groups = mine // ROWS
    batches = groups // 2
    tile = ROWS // 2
    chan_count = lax.axis_size("chan")
    vmem = pl.BlockSpec(memory_space=pltpu.VMEM)
    f32 = jnp.float32
    dma = pltpu.SemaphoreType.DMA
    relayed = len(RELAYED)
    tables_in = (window, first_all, second_all, twist, mirror)
    packed = pl.pallas_call(
        functools.partial(welch_kernel, 1.0 / (segments * energy)),
        in_specs=[pl.BlockSpec(memory_space=pl.ANY)] * 6,
        out_specs=pl.BlockSpec(memory_space=pl.ANY),
        out_shape=jax.ShapeDtypeStruct((2 * chan_rows + ROWS, ROOT), f32),
        scratch_shapes=[pltpu.VMEM(table.shape, table.dtype) for table in tables_in]
        + [
            pltpu.VMEM((2 * chan_rows, ROOT), f32),
            pltpu.VMEM((ROWS, ROOT), f32),
            dma((len(tables_in),)),
            dma((2,)),
            pltpu.VMEM((mine, CORES * seg_len + half_len), f32),
            pltpu.VMEM((relayed, CORES, ROWS, half_len), f32),
            pltpu.VMEM((pairs, SPAN, SPAN, ROWS, ROOT), f32),
            pltpu.VMEM(((pairs + 2) * ROWS, ROOT), f32),
            pltpu.VMEM(((pairs + 2) * ROWS, ROOT), f32),
            pltpu.VMEM((3, groups, tile, SPAN, ROWS, ROOT), f32),
            pltpu.VMEM((3, groups, tile, ROWS, ROOT), f32),
            pltpu.VMEM((SPAN * SPAN, 2, ROWS, ROOT), f32),
            pltpu.VMEM((SPAN, SPAN, 2, ROWS, ROOT), f32),
            pltpu.VMEM((SPAN, SPAN, ROWS, ROOT), f32),
            pltpu.VMEM((chan_count, SPAN, SPAN, ROWS, ROOT), f32),
            pltpu.VMEM((ROOT, ROOT), f32),
            pltpu.VMEM((ROWS * ROOT, ROOT), f32),
            pltpu.VMEM((ROWS * 2 * CORES * HALF, 4 * ROOT), jnp.bfloat16),
            pltpu.VMEM((2 * CORES * ROWS, 6 * ROOT), jnp.bfloat16),
            pltpu.VMEM((ROWS * HALF, ROOT), f32),
            dma((groups,)),
            dma(()),
            dma((groups,)),
            dma(()),
            dma((2, batches)),
            dma(()),
            dma((relayed, CORES)),
            dma(()),
            dma((3, groups)),
            dma(()),
            dma((3, groups)),
            dma(()),
            dma(()),
            dma(()),
            dma((batches,)),
            dma((chan_count,)),
            dma((chan_count,)),
        ],
        compiler_params=pltpu.CompilerParams(
            collective_id=0, has_side_effects=True, vmem_limit_bytes=60 * 2**20
        ),
        name="welch",
    )(strain, *tables_in)
    power, nyquist, mean_power = pl.pallas_call(
        finish_kernel,
        in_specs=[vmem],
        out_specs=[vmem] * 3,
        out_shape=[
            jax.ShapeDtypeStruct((chan_rows, 2 * ROOT), f32),
            jax.ShapeDtypeStruct((1, chan_rows), f32),
            jax.ShapeDtypeStruct((1, 2 * ROOT), f32),
        ],
        name="finish",
    )(packed)
    return (power, nyquist.reshape(-1), mean_power.reshape(-1))


def solution(mesh):
    in_specs = (P("chan", "tm"),)
    out_specs = (P("chan", "tm"), P("chan"), P("tm"))
    return jax.shard_map(
        per_device, mesh=mesh, in_specs=in_specs, out_specs=out_specs, check_vma=False
    )
```

```python
import functools

import jax
import jax.numpy as jnp
import numpy as np
from jax import lax
from jax.experimental import pallas as pl
from jax.experimental.pallas import tpu as pltpu
from jax.sharding import PartitionSpec as P

ROOT = 128
HALF = ROOT // 2
ROWS = 8


def split_np(table):
    table = table.astype(np.float32)
    high = table.astype(jnp.bfloat16)
    low = (table - high.astype(np.float32)).astype(jnp.bfloat16)
    return high, low


@functools.cache
def tables(tm_count):
    pos = np.arange(ROOT)
    short = 2.0 * np.pi * (np.outer(pos, pos) % ROOT) / ROOT
    cos_s, sin_s = np.cos(short), np.sin(short)
    first = np.concatenate([cos_s[:HALF], -sin_s[:HALF]], axis=0)
    first_hi, first_lo = split_np(first)
    first_all = np.concatenate(
        [
            np.concatenate([first_hi, first_hi], axis=1),
            np.concatenate([first_lo, first_lo], axis=1),
        ],
        axis=0,
    )
    bands = np.arange(HALF).reshape(tm_count, HALF // tm_count)
    order = np.concatenate([bands, ROOT - 1 - bands], axis=1).reshape(-1)
    cos_o, sin_o = cos_s[:, order], sin_s[:, order]
    second = np.concatenate(
        [np.concatenate([cos_o, -sin_o], axis=1), np.concatenate([sin_o, cos_o], axis=1)], axis=0
    )
    second_hi, second_lo = split_np(second)
    second_all = np.concatenate([second_hi, second_hi, second_lo], axis=0)
    long = 2.0 * np.pi * np.outer(np.arange(HALF + ROWS), pos) / (ROOT * ROOT)
    twist = np.concatenate([np.cos(long), np.sin(long)], axis=1).astype(np.float32)
    mirror = np.zeros((2 * ROOT, 2 * ROOT), np.float32)
    for side in range(2):
        for k in range(HALF):
            mirror[side * HALF + k, side * ROOT + k] = 1.0
            mirror[ROOT + side * HALF + k, side * ROOT + (ROOT - k if k else HALF)] = 1.0
    seg_len = ROOT * ROOT
    window = 0.5 - 0.5 * np.cos(2.0 * np.pi * np.arange(seg_len) / seg_len)
    energy = float(np.sum(window * window))
    return first_all, second_all, twist, window.reshape(ROOT, ROOT).astype(np.float32), mirror.astype(jnp.bfloat16), energy


def split(value):
    high = value.astype(jnp.bfloat16)
    low = (value - high.astype(jnp.float32)).astype(jnp.bfloat16)
    return high, low


SPAN = 4
CORES = 2


RELAYED = (2, 4, 5)
RELAY_AT = (2, 5, 7)
HELD = 3
CHUNK = 4
LATE = ((7, 0, 4), (8, 4, 6), (9, 6, 7), (10, 7, 9), (11, 9, 10))
SHORT = 8
X_START = ((9, 0, 4), (10, 4, 6), (11, 6, 8))


def half_sum(ref):
    parts = [ref[:, ROOT * a : ROOT * (a + 1)] for a in range(HALF)]
    while len(parts) > 1:
        parts = [parts[n] + parts[n + 1] for n in range(0, len(parts), 2)]
    return jnp.sum(parts[0], axis=1, keepdims=True)


def window_piece(piece, mean, consts, buf, ebuf, seg):
    window_ref, _, _, twist_ref = consts
    base = (seg % 2) * ROWS * ROOT
    mean = jnp.broadcast_to(mean, (ROWS, ROOT))
    even = jnp.zeros((ROWS, ROOT), jnp.float32)
    odd = jnp.zeros((ROWS, ROOT), jnp.float32)
    for a in range(ROOT):
        tile = (piece[:, ROOT * a : ROOT * (a + 1)] - mean) * window_ref[a : a + 1, :]
        buf[base + ROWS * a : base + ROWS * (a + 1), :] = tile
        if a % 2 == 0:
            even = even + tile
        else:
            odd = odd + tile
    alt = even - odd
    sign = (1 - 2 * (lax.broadcasted_iota(jnp.int32, (ROWS, ROOT), 1) % 2)).astype(jnp.float32)
    edge = jnp.sum((even + odd) * sign, axis=1, keepdims=True)
    turn = twist_ref[HALF : HALF + 1, :]
    high, low = split(jnp.concatenate([alt * turn[:, :ROOT], -alt * turn[:, ROOT:]], axis=1))
    ebuf[seg * ROWS : (seg + 1) * ROWS, :] = jnp.concatenate([high, low, high], axis=1)
    return edge * edge


def stage_one(seg, r, consts, buf, zbuf):
    _, first_ref, _, twist_ref = consts
    base = (seg % 2) * ROWS * ROOT
    cos_t, sin_t = twist_ref[:HALF, :ROOT], twist_ref[:HALF, ROOT:]
    pair = jnp.concatenate(
        [buf[pl.ds(base + r + s, ROOT, stride=ROWS), :] for s in range(2)], axis=1
    )
    high, low = split(pair)
    right = jnp.concatenate([high, low], axis=0)
    out = jnp.dot(first_ref[:ROOT, :], right, preferred_element_type=jnp.float32)
    out = out + jnp.dot(first_ref[ROOT:, :], right, preferred_element_type=jnp.float32)
    for s in range(2):
        re = out[:HALF, s * ROOT : (s + 1) * ROOT]
        im = out[HALF:, s * ROOT : (s + 1) * ROOT]
        z_hi, z_lo = split(
            jnp.concatenate([re * cos_t + im * sin_t, im * cos_t - re * sin_t], axis=1)
        )
        at = (seg * ROWS + r + s) * HALF
        zbuf[at : at + HALF, 0 : 2 * ROOT] = z_hi
        zbuf[at : at + HALF, 2 * ROOT :] = z_lo


def squares(left, right):
    out = jnp.dot(left, right, preferred_element_type=jnp.float32)
    return out[:, :ROOT] * out[:, :ROOT] + out[:, ROOT:] * out[:, ROOT:]


def stage_two(seg, r, count, weight, consts, zbuf, psum):
    at = slice((seg * ROWS + r) * HALF, (seg * ROWS + r + count) * HALF)
    left = jnp.concatenate([zbuf[at, :], zbuf[at, : 2 * ROOT]], axis=1)
    power = squares(left, consts[2][...])
    if weight is not None:
        power = weight * power
    to = slice(r * HALF, (r + count) * HALF)
    psum[to, :] = power if seg == 0 else psum[to, :] + power


def group_sums(side, rows, on, wait_halo, consts, scratch):
    second_ref = consts[2]
    buf, zbuf, ebuf, psum = scratch
    half_len = ROOT * HALF
    segs = 2 * CORES
    lane = lax.broadcasted_iota(jnp.int32, (ROWS, ROOT), 1)

    def window(start, length):
        return rows.at[:, pl.ds(pl.multiple_of(start, half_len), length)]

    own = side * half_len
    totals = [half_sum(window(own + h * half_len, half_len)) for h in range(segs)]
    inverse = 1.0 / (2 * half_len)
    nyq = jnp.zeros((ROWS, 1), jnp.float32)
    for seg in range(segs - 1):
        nyq = nyq + window_piece(
            window(own + seg * half_len, 2 * half_len), (totals[seg] + totals[seg + 1]) * inverse,
            consts, buf, ebuf, seg,
        )
        for r in range(0, ROWS, 2):
            stage_one(seg, r, consts, buf, zbuf)
            if seg > 0 and (r + 2) % CHUNK == 0:
                stage_two(seg - 1, r + 2 - CHUNK, CHUNK, None, consts, zbuf, psum)
    wait_halo()
    last = segs - 1
    near = jnp.where(side == 0, totals[-1], totals[0])
    far = half_sum(window((1 - side) * segs * half_len, half_len))
    nyq = nyq + on * window_piece(
        window((1 - side) * last * half_len, 2 * half_len), (near + far) * inverse, consts, buf, ebuf, last
    )
    for r in range(0, ROWS, 2):
        stage_one(last, r, consts, buf, zbuf)
        if (r + 2) % CHUNK == 0:
            stage_two(last - 1, r + 2 - CHUNK, CHUNK, None, consts, zbuf, psum)
    for r in range(0, ROWS, CHUNK):
        stage_two(last, r, CHUNK, on, consts, zbuf, psum)
    power = squares(ebuf[...], second_ref[...])
    mixed = power[:ROWS]
    for seg in range(1, last):
        mixed = mixed + power[seg * ROWS : (seg + 1) * ROWS]
    mixed = mixed + on * power[last * ROWS :]
    first_rows = pl.ds(0, ROWS, stride=HALF)
    psum[first_rows, :] = jnp.where(lane % SPAN >= SPAN // 2, mixed, psum[first_rows, :])
    return nyq


def welch_kernel(
    scale, strain_ref, window_hbm, first_hbm, second_hbm, twist_hbm, mirror_hbm, packed_ref,
    window_ref, first_ref, second_ref, twist_ref, mirror_ref, power_box, small_box, table_sem, out_sem,
    data, relay_box, sums, fin, from_partner, z_in, x_in, direct_in, direct_out, group_sum, group_in, nyq_rows,
    buf, zbuf, ebuf, psum,
    load_sem, swap_send, swap_recv, halo_send, halo_recv, relay_send, relay_recv,
    z_send, z_recv, x_send, x_recv, direct_send, direct_recv, core_send, core_recv, mean_send, mean_recv,
):
    chan, chan_count = lax.axis_index("chan"), lax.axis_size("chan")
    me = lax.axis_index("tm")
    core = lax.rem(me, CORES)
    chip = me // CORES
    chips = lax.axis_size("tm") // CORES
    z, x = chip // SPAN, lax.rem(chip, SPAN)
    half_len = ROOT * HALF
    block_len = 2 * half_len
    mine = data.shape[0]
    groups = mine // ROWS
    tile = ROWS // 2
    batches = groups // 2
    ringed = groups
    size = tile * ROWS
    inner = jnp.logical_and(x > 0, x < SPAN - 1)
    has_left, has_right = chip > 0, chip < chips - 1
    exists = (has_right, has_left)

    def as_int(flag):
        return flag.astype(jnp.int32)

    def device(chip_index, core_index):
        return {"tm": chip_index * CORES + core_index}

    def z_peer(step):
        return device(lax.rem(z + step + SPAN, SPAN) * SPAN + x, core)

    def x_peer(step):
        return device(z * SPAN + lax.rem(x + step + SPAN, SPAN), core)

    partner = device(chip, 1 - core)
    toward = 2 * core - 1
    sends_halo = jnp.where(core == 0, as_int(has_left), as_int(has_right)) == 1
    at_column = jnp.logical_or(x == 0, x == SPAN - 1)
    has_next_row = jnp.where(core == 0, as_int(z > 0), as_int(z < SPAN - 1)) == 1
    linked = jnp.logical_and(at_column, has_next_row)
    crosses = jnp.logical_and(linked, x == (SPAN - 1) * core)
    relays = jnp.logical_and(linked, x == (SPAN - 1) * (1 - core))
    faces = x == (SPAN - 1) * (1 - core)
    next_row = device(chip + toward * SPAN, 1 - core)

    def across(core_index):
        return device(z * SPAN + (SPAN - 1) - x, core_index)

    def remote(source, target, send, recv, where):
        return pltpu.make_async_remote_copy(
            src_ref=source, dst_ref=target, send_sem=send, recv_sem=recv,
            device_id=where, device_id_type=pl.DeviceIdType.MESH,
        )

    def strip(g):
        return pl.ds(pl.multiple_of(g * ROWS, ROWS), ROWS)

    def columns(g, side):
        start = side * half_len + core * block_len
        return pl.ds(pl.multiple_of(start, half_len), block_len)

    def load(g):
        rows = pl.ds(pl.multiple_of(core * mine + g * ROWS, ROWS), ROWS)
        place = data.at[strip(g), columns(g, lax.rem(g + core, 2))]
        return pltpu.make_async_copy(strain_ref.at[rows], place, load_sem.at[g])

    def swap(g):
        rows = pl.ds(pl.multiple_of((1 - core) * mine + g * ROWS, ROWS), ROWS)
        place = data.at[strip(g), columns(g, lax.rem(g + 1 - core, 2))]
        return remote(strain_ref.at[rows], place, swap_send, swap_recv.at[g], partner)

    def halo_group(n, side, to):
        return 2 * n + lax.rem(side + to, 2)

    def halo_place(n, side, to):
        start = (1 - side) * 2 * CORES * half_len
        return data.at[strip(halo_group(n, side, to)), pl.ds(pl.multiple_of(start, half_len), half_len)]

    def halo_source(n, to):
        return strain_ref.at[
            pl.ds(pl.multiple_of(to * mine + halo_group(n, core, to) * ROWS, ROWS), ROWS),
            pl.ds(pl.multiple_of(core * half_len, half_len), half_len),
        ]

    def halo_copy(n, to):
        return remote(
            halo_source(n, to), halo_place(n, core, to), halo_send, halo_recv.at[core, n],
            device(chip + toward, to),
        )

    def relay_copy(k, to):
        n = RELAYED[k]
        return remote(
            halo_source(n, to), relay_box.at[k, to], halo_send, relay_recv.at[k, to], next_row
        )

    def relay_on(k, to):
        n = RELAYED[k]
        return remote(
            relay_box.at[k, to], halo_place(n, 1 - core, to), relay_send,
            halo_recv.at[1 - core, n], across(to),
        )

    def halo_arrival(n, side):
        block = halo_place(n, side, core)
        return remote(block, block, halo_send, halo_recv.at[side, n], partner)

    barrier = pltpu.get_barrier_semaphore()

    def greet(where):
        pl.semaphore_signal(barrier, inc=1, device_id=where, device_id_type=pl.DeviceIdType.MESH)

    def chan_peer(k):
        return {"chan": lax.rem(chan + k, chan_count)}

    def chip_peer(k):
        far_z, far_x = lax.rem(z + k // SPAN, SPAN), lax.rem(x + k % SPAN, SPAN)
        return far_z, far_x, device(far_z * SPAN + far_x, core)

    greet(partner)
    for k in range(1, SPAN * SPAN):
        greet(chip_peer(k)[2])
    for k in range(1, chan_count):
        greet(chan_peer(k))
    for flag, shift, both in ((has_left, -1, 0), (has_right, 1, 1)):
        @pl.when(flag)
        def _():
            greet(device(chip + shift, 1 - both))

            @pl.when(core == both)
            def _():
                greet(device(chip + shift, both))

    @pl.when(linked)
    def _():
        greet(next_row)

    @pl.when(faces)
    def _():
        greet(across(1 - core))

    tables_in = [
        pltpu.make_async_copy(source, target, table_sem.at[n])
        for n, (source, target) in enumerate(
            zip(
                (window_hbm, first_hbm, second_hbm, twist_hbm, mirror_hbm),
                (window_ref, first_ref, second_ref, twist_ref, mirror_ref),
            )
        )
    ]
    load(0).start()
    for table in tables_in:
        table.start()

    @pl.loop(1, groups)
    def _(g):
        load(g).start()

    left_count = as_int(has_left) * (2 - core)
    right_count = as_int(has_right) * (1 + core)
    pl.semaphore_wait(
        barrier,
        left_count + right_count + as_int(linked) + as_int(faces) + SPAN * SPAN + chan_count - 1,
    )

    for n in range(batches):
        for side in range(2):
            swap(2 * n + side).start()

        @pl.when(sends_halo)
        def _():
            for turn in range(CORES):
                to = lax.rem(core + turn, CORES)
                if n in RELAYED:
                    @pl.when(crosses)
                    def _():
                        relay_copy(RELAYED.index(n), to).start()

                    @pl.when(jnp.logical_not(crosses))
                    def _():
                        halo_copy(n, to).start()
                elif n == HELD:
                    @pl.when(jnp.logical_not(crosses))
                    def _():
                        halo_copy(n, to).start()
                else:
                    halo_copy(n, to).start()

    nyq_rows[...] = jnp.zeros_like(nyq_rows)
    group_sum[...] = jnp.zeros_like(group_sum)
    for table in tables_in:
        table.wait()
    consts = (window_ref, first_ref, second_ref, twist_ref)
    scratch = (buf, zbuf, ebuf, psum)

    def slab(i, size):
        return pl.ds(pl.multiple_of(i * size, size), size)

    def way(i):
        return 1 - 2 * lax.rem(i, 2)

    def z_block(i, step):
        return sums.at[slab(i, tile), lax.rem(z + step + SPAN, SPAN)]

    def x_block(i, step):
        return sums.at[slab(i, tile), z, lax.rem(x + step + SPAN, SPAN)]

    def ring(kind, i, block, inbox, send, recv, peer):
        d = way(i)
        step, hop = ((2, d), (-d, -d), (d, d))[kind]
        return remote(block(i, step), inbox.at[kind, i], send, recv.at[kind, i], peer(hop))

    def z_copy(kind, i):
        return ring(kind, i, z_block, z_in, z_send, z_recv, z_peer)

    def x_copy(kind, i):
        return ring(kind, i, x_block, x_in, x_send, x_recv, x_peer)

    def core_copy(i):
        count = 2 * size + (2 * ROWS if i == batches - 1 else 0)
        rows = pl.ds(i * 2 * size, count)
        return remote(fin.at[rows], from_partner.at[rows], core_send, core_recv.at[i], partner)

    def direct_copy(k):
        far_z, far_x, where = chip_peer(k)
        return remote(direct_out.at[far_z, far_x], direct_in.at[k], direct_send, direct_recv, where)

    def direct_all():
        box = direct_in.at[pl.ds(1, SPAN * SPAN - 1)]
        return remote(box, box, direct_send, direct_recv, partner)

    def send_direct():
        for k in (10, 6, 9, 11, 14, 2, 8, 5, 7, 13, 15, 1, 3, 4, 12):
            direct_copy(k).start()

    def sum_direct():
        direct_all().wait_recv()
        total = jnp.zeros((2, ROWS, ROOT), jnp.float32)
        for far_z in range(SPAN):
            for far_x in range(SPAN):
                k = lax.rem(z - far_z + SPAN, SPAN) * SPAN + lax.rem(x - far_x + SPAN, SPAN)
                total = total + direct_in[k]
        fin[pl.ds(groups * size, 2 * ROWS), :] = total.reshape(2 * ROWS, ROOT)

    def chan_copy(k):
        return remote(group_sum, group_in.at[k], mean_send.at[k], mean_recv.at[k], chan_peer(k))

    def chan_begin():
        for k in (2, 1, 3):
            chan_copy(k).start()
        group_in[0] = group_sum[...]

    def chan_collect():
        for k in range(1, chan_count):
            chan_copy(k).wait_recv()
        total = group_in[lax.rem(chan + chan_count, chan_count)]
        for source in range(1, chan_count):
            total = total + group_in[lax.rem(chan - source + chan_count, chan_count)]
        direct_out[:, :, 1] = total
        direct_in[0] = direct_out[z, x]

    def begin(copy, i):
        copy(0, i).start()
        copy(1, i).start()

    def advance(copy, block, inbox, i):
        copy(0, i).wait_recv()
        target = block(i, way(i))
        target[...] = target[...] + inbox[0, i]
        copy(2, i).start()

    def collect(copy, block, inbox, i):
        copy(1, i).wait_recv()
        copy(2, i).wait_recv()
        return block(i, 0)[...] + inbox[1, i] + inbox[2, i]

    def z_advance(i):
        advance(z_copy, z_block, z_in, i)

    def z_collect(i):
        z_block(i, 0)[...] = collect(z_copy, z_block, z_in, i)

    def short_copy(k, i):
        return remote(x_block(i, k), x_in.at[k - 1, i], x_send, x_recv.at[k - 1, i], x_peer(k))

    def short_begin(i):
        for k in (2, 1, 3):
            short_copy(k, i).start()

    def short_collect(i):
        total = x_block(i, 0)[...]
        for k in (1, 3, 2):
            short_copy(k, i).wait_recv()
            total = total + x_in[k - 1, i]
        fin[pl.ds(i * size, size), :] = total.reshape(size, ROOT)

    def x_advance(i):
        advance(x_copy, x_block, x_in, i)

    def x_collect(i):
        rows = pl.ds(pl.multiple_of(i * size, size), size)
        fin[rows, :] = collect(x_copy, x_block, x_in, i).reshape(size, ROOT)

    @pl.loop(0, groups)
    def _(t):
        side = lax.rem(t + core, 2)
        here = jnp.where(side == 0, as_int(has_right), as_int(has_left))
        load(t).wait()
        swap(t).wait_recv()

        for k in range(len(RELAYED)):
            @pl.when(jnp.logical_and(relays, t == RELAY_AT[k]))
            def _():
                for turn in range(CORES):
                    to = lax.rem(1 - core + turn, CORES)
                    relay_copy(k, to).wait_recv()
                    relay_on(k, to).start()

        @pl.when(jnp.logical_and(crosses, t == HELD))
        def _():
            for turn in range(CORES):
                halo_copy(HELD, lax.rem(core + turn, CORES)).start()

        def wait_halo():
            @pl.when(jnp.logical_and(inner, t >= 2))
            def _():
                z_advance(t - 2)

            for at, first, last in LATE:
                @pl.when(jnp.logical_and(jnp.logical_not(inner), t == at))
                def _():
                    @pl.loop(first, last)
                    def _(i):
                        z_advance(i)

            for at, first, last in X_START:
                @pl.when(t == at)
                def _():
                    @pl.loop(first, last)
                    def _(i):
                        z_collect(i)
                        begin(x_copy, i)

            @pl.when(t == groups - 1)
            def _():
                @pl.loop(0, 4)
                def _(i):
                    x_advance(i)

            @pl.when(here == 1)
            def _():
                halo_arrival(t // 2, side).wait_recv()

            @pl.when(here == 0)
            def _():
                place = halo_place(t // 2, side, core)
                place[...] = jnp.zeros((ROWS, half_len), jnp.float32)

        nyq = group_sums(side, data.at[strip(t)], here.astype(jnp.float32), wait_halo, consts, scratch)
        nyq_rows[strip(t), :] = jnp.broadcast_to(nyq, (ROWS, ROOT))
        added = group_sum[...]
        for p in range(tile):
            turned = jnp.transpose(psum[p * ROOT : (p + 1) * ROOT, :]).reshape(sums.shape[1:])
            sums[t * tile + p] = turned
            added = added + turned
        group_sum[...] = added

        begin(z_copy, t)

    chan_begin()
    direct_out[:, :, 0] = jnp.broadcast_to(
        jnp.transpose(nyq_rows[...])[:ROWS].reshape(1, 1, ROWS, ROOT), (SPAN, SPAN, ROWS, ROOT)
    )
    z_advance(10)
    x_advance(4)
    x_advance(5)
    z_collect(8)
    short_begin(8)
    z_collect(9)
    short_begin(9)
    x_advance(6)
    x_advance(7)
    z_advance(11)
    z_collect(10)
    short_begin(10)
    chan_collect()
    send_direct()
    for i in range(4):
        x_collect(i)
    core_copy(0).start()
    core_copy(1).start()
    z_collect(11)
    short_begin(11)
    x_collect(4)
    x_collect(5)
    core_copy(2).start()
    x_collect(6)
    x_collect(7)
    core_copy(3).start()
    short_collect(8)
    short_collect(9)
    core_copy(4).start()

    lanes = lax.broadcasted_iota(jnp.int32, (1, ROOT), 1)
    factors = [jnp.where(jnp.logical_and(lanes == 0, me + j == 0), scale, 2.0 * scale) for j in range(2)]

    def unfold(both):
        high = both.astype(jnp.bfloat16)
        middle = (both - high.astype(jnp.float32)).astype(jnp.bfloat16)
        low = (both - high.astype(jnp.float32) - middle.astype(jnp.float32)).astype(jnp.bfloat16)
        parts = [jnp.dot(part, mirror_ref[...], preferred_element_type=jnp.float32) for part in (low, middle, high)]
        return parts[0] + parts[1] + parts[2]

    def spread(block, owner, first, count):
        for j in range(2):
            both = jnp.concatenate(
                [block[pl.ds(SPAN * core + j + shift + first * ROWS, count, stride=ROWS), :] for shift in (0, 2)],
                axis=1,
            )
            placed = unfold(both)
            for half in range(2):
                at = j * CORES * mine + owner * mine + 2 * first + half
                power_box[pl.ds(at, count, stride=2), :] = placed[:, half * ROOT : (half + 1) * ROOT] * factors[j]

    most = 10 * tile
    spread(fin, core, 0, most)
    short_collect(10)
    for b in range(batches - 1):
        core_copy(b).wait_recv()
    spread(from_partner, 1 - core, 0, most)
    sum_direct()
    short_collect(11)
    core_copy(5).start()
    spread(fin, core, most, groups * tile - most)
    core_copy(batches - 1).wait_recv()
    spread(from_partner, 1 - core, most, groups * tile - most)
    power_out = pltpu.make_async_copy(power_box, packed_ref.at[: power_box.shape[0]], out_sem.at[0])
    power_out.start()

    ends = [ref[groups * size : groups * size + 1, :] * scale for ref in (fin, from_partner)]
    parts = [jnp.where(core == source, ends[0], ends[1]) for source in range(CORES)]
    moved = pltpu.roll(parts[1], mine, 1)
    small_box[...] = jnp.zeros_like(small_box)
    small_box[0:1, :] = jnp.where(lanes < mine, parts[0], moved)
    small_box[1:2, :] = moved
    rows = []
    for j in range(SPAN):
        at = pl.ds(groups * size + ROWS + SPAN * core + j, 1)
        here, there = fin[at, :], from_partner[at, :]
        rows.append(jnp.where(core == 0, here, there) + jnp.where(core == 0, there, here))
    placed = unfold(
        jnp.concatenate(
            [jnp.concatenate([rows[j], rows[j + 2]], axis=1) for j in range(2)]
            + [jnp.zeros((ROWS - 2, 2 * ROOT), jnp.float32)],
            axis=0,
        )
    )
    placed = placed[:, :ROOT] + placed[:, ROOT:]
    for j in range(2):
        small_box[2 + j : 3 + j, :] = placed[j : j + 1] * (factors[j] * (1.0 / (CORES * mine * chan_count)))
    small_out = pltpu.make_async_copy(small_box, packed_ref.at[power_box.shape[0] :], out_sem.at[1])
    small_out.start()

    def sent(box, send):
        remote(box, box, send, core_recv.at[0], partner).wait_send()

    sent(strain_ref.at[pl.ds(0, mine)], swap_send)
    sent(z_in, z_send)
    sent(x_in, x_send)
    sent(fin, core_send)
    direct_all().wait_send()

    @pl.when(sends_halo)
    def _():
        sent(strain_ref.at[pl.ds(0, mine), pl.ds(0, half_len)], halo_send)

    @pl.when(relays)
    def _():
        sent(relay_box, relay_send)

    for k in range(1, chan_count):
        chan_copy(k).wait_send()
    power_out.wait()
    small_out.wait()


def finish_kernel(packed_ref, power_ref, nyquist_ref, mean_ref):
    chan_rows = power_ref.shape[0]
    for j in range(2):
        power_ref[:, j * ROOT : (j + 1) * ROOT] = packed_ref[j * chan_rows : (j + 1) * chan_rows, :]
        mean_ref[:, j * ROOT : (j + 1) * ROOT] = packed_ref[2 * chan_rows + 2 + j : 2 * chan_rows + 3 + j, :]
    nyquist_ref[:, :ROOT] = packed_ref[2 * chan_rows : 2 * chan_rows + 1, :]
    nyquist_ref[:, ROOT:] = packed_ref[2 * chan_rows + 1 : 2 * chan_rows + 2, : chan_rows - ROOT]


def per_device(strain):
    chan_rows, time_width = strain.shape
    seg_len = ROOT * ROOT
    half_len = seg_len // 2
    tm_count = lax.axis_size("tm")
    mine = chan_rows // CORES
    assert time_width == seg_len and tm_count == SPAN * SPAN * CORES and mine == 12 * ROWS
    segments = 2 * tm_count - 1
    first_all, second_all, twist, window, mirror, energy = tables(tm_count)
    pairs = mine // 2
    groups = mine // ROWS
    batches = groups // 2
    tile = ROWS // 2
    chan_count = lax.axis_size("chan")
    vmem = pl.BlockSpec(memory_space=pltpu.VMEM)
    f32 = jnp.float32
    dma = pltpu.SemaphoreType.DMA
    relayed = len(RELAYED)
    tables_in = (window, first_all, second_all, twist, mirror)
    packed = pl.pallas_call(
        functools.partial(welch_kernel, 1.0 / (segments * energy)),
        in_specs=[pl.BlockSpec(memory_space=pl.ANY)] * 6,
        out_specs=pl.BlockSpec(memory_space=pl.ANY),
        out_shape=jax.ShapeDtypeStruct((2 * chan_rows + ROWS, ROOT), f32),
        scratch_shapes=[pltpu.VMEM(table.shape, table.dtype) for table in tables_in]
        + [
            pltpu.VMEM((2 * chan_rows, ROOT), f32),
            pltpu.VMEM((ROWS, ROOT), f32),
            dma((len(tables_in),)),
            dma((2,)),
            pltpu.VMEM((mine, CORES * seg_len + half_len), f32),
            pltpu.VMEM((relayed, CORES, ROWS, half_len), f32),
            pltpu.VMEM((pairs, SPAN, SPAN, ROWS, ROOT), f32),
            pltpu.VMEM(((pairs + 2) * ROWS, ROOT), f32),
            pltpu.VMEM(((pairs + 2) * ROWS, ROOT), f32),
            pltpu.VMEM((3, groups, tile, SPAN, ROWS, ROOT), f32),
            pltpu.VMEM((3, groups, tile, ROWS, ROOT), f32),
            pltpu.VMEM((SPAN * SPAN, 2, ROWS, ROOT), f32),
            pltpu.VMEM((SPAN, SPAN, 2, ROWS, ROOT), f32),
            pltpu.VMEM((SPAN, SPAN, ROWS, ROOT), f32),
            pltpu.VMEM((chan_count, SPAN, SPAN, ROWS, ROOT), f32),
            pltpu.VMEM((ROOT, ROOT), f32),
            pltpu.VMEM((2 * ROWS * ROOT, ROOT), f32),
            pltpu.VMEM((ROWS * 2 * CORES * HALF, 4 * ROOT), jnp.bfloat16),
            pltpu.VMEM((2 * CORES * ROWS, 6 * ROOT), jnp.bfloat16),
            pltpu.VMEM((ROWS * HALF, ROOT), f32),
            dma((groups,)),
            dma(()),
            dma((groups,)),
            dma(()),
            dma((2, batches)),
            dma(()),
            dma((relayed, CORES)),
            dma(()),
            dma((3, groups)),
            dma(()),
            dma((3, groups)),
            dma(()),
            dma(()),
            dma(()),
            dma((batches,)),
            dma((chan_count,)),
            dma((chan_count,)),
        ],
        compiler_params=pltpu.CompilerParams(
            collective_id=0, has_side_effects=True, vmem_limit_bytes=60 * 2**20
        ),
        name="welch",
    )(strain, *tables_in)
    power, nyquist, mean_power = pl.pallas_call(
        finish_kernel,
        in_specs=[vmem],
        out_specs=[vmem] * 3,
        out_shape=[
            jax.ShapeDtypeStruct((chan_rows, 2 * ROOT), f32),
            jax.ShapeDtypeStruct((1, chan_rows), f32),
            jax.ShapeDtypeStruct((1, 2 * ROOT), f32),
        ],
        name="finish",
    )(packed)
    return (power, nyquist.reshape(-1), mean_power.reshape(-1))


def solution(mesh):
    in_specs = (P("chan", "tm"),)
    out_specs = (P("chan", "tm"), P("chan"), P("tm"))
    return jax.shard_map(
        per_device, mesh=mesh, in_specs=in_specs, out_specs=out_specs, check_vma=False
    )
```
